8 devices in a mesh: rep: 2 (over y, z), dp: 4 (over x, core).
Axes of the slice: x: 2, y: 2, z: 1, core: 2. Of those that a mesh axis runs over, the one named last changes fastest.
Arguments:
- x: bfloat16 [8, 2048, 768], P(('rep', 'dp')), parts along dimension 0
- dy: bfloat16 [8, 2048, 768], P(('rep', 'dp')), parts along dimension 0
- w_gate: bfloat16 [2, 768, 3072], P(None, 'dp')
- w_up: bfloat16 [2, 768, 3072], P(None, 'dp')
- w_down: bfloat16 [2, 3072, 768], P(None, 'dp')
Outputs:
- output 1: bfloat16 [8, 2048, 768], P(('rep', 'dp')), parts along dimension 0
- output 2: bfloat16 [4, 768, 3072], P('rep', 'dp'), parts along dimension 0
- output 3: bfloat16 [4, 768, 3072], P('rep', 'dp'), parts along dimension 0
- output 4: bfloat16 [4, 3072, 768], P('rep', 'dp'), parts along dimension 0
There are 2 independent parts. The reference program is written for one: setup_inputs(seed, part) draws one part's arguments, and reference() takes and returns one part's arrays. A program takes and returns all parts, laid end to end along the dimension named above; an argument that names none is the same for every part.
All inputs are finite; a program needn't handle non-finite values.
Results may differ from the reference program's by a relative error of at most 0.018.
Values are sent between devices in bfloat16 or wider.
A program may use at most 2 GiB of HBM per device.

```python
import jax
import jax.numpy as jnp
from jax import lax

SEQUENCES = 4
TOKENS = 2048
D = 768
FF = 3072
LAYERS = 2
NAMES = ("w_gate", "w_up", "w_down")
SHAPES = {"w_gate": (LAYERS, D, FF), "w_up": (LAYERS, D, FF), "w_down": (LAYERS, FF, D)}


def bump(key, n, height):
    away = (jnp.arange(n, dtype=jnp.int32) - jax.random.randint(key, (), 0, n, jnp.int32)) % n
    return jnp.where(away < n // 8, height, 1.0)


def together(key, own, strength):
    shared = jax.random.normal(key, own.shape[1:], jnp.float32)
    return (own + strength * shared) * lax.rsqrt(1 + strength * strength)


def setup_inputs(seed: int = 0, part: int = 0) -> dict:
    kx, kdy, ka, kb, kz, kf, kh, kl, *kw = jax.random.split(jax.random.key(seed), 8 + len(NAMES))
    kx, kdy, ka, kb = (jax.random.fold_in(k, part) for k in (kx, kdy, ka, kb))
    shape = (SEQUENCES, TOKENS, D)
    much_x, much_dy = jax.random.uniform(kz, (2,), jnp.float32, 0.0, 1.0)
    layers = 2.0 ** jax.random.uniform(kl, (LAYERS, 1, 1), jnp.float32, -1.0, 1.0)
    x = together(ka, jax.random.normal(kx, shape, jnp.float32), much_x) * bump(kf, D, 4.0)
    dy = together(kb, jax.random.normal(kdy, shape, jnp.float32), much_dy)
    drawn = {"x": x.astype(jnp.bfloat16), "dy": (dy * (SEQUENCES * TOKENS) ** -0.5).astype(jnp.bfloat16)}
    for key, name in zip(kw, NAMES, strict=True):
        w = jax.random.normal(key, SHAPES[name], jnp.float32) * SHAPES[name][1] ** -0.5
        drawn[name] = (w * {"w_gate": 1.0, "w_up": bump(kh, FF, 4.0), "w_down": layers}[name]).astype(jnp.bfloat16)
    return drawn


def matmul(a, w):
    return jnp.dot(a, w, preferred_element_type=jnp.float32).astype(jnp.bfloat16)


def normed(h):
    wide = h.astype(jnp.float32)
    scale = lax.rsqrt(jnp.mean(wide**2, -1, keepdims=True) + 1e-6)
    return (wide * scale).astype(jnp.bfloat16)


def layer(h, w):
    a = normed(h)
    gate = jnp.dot(a, w["w_gate"], preferred_element_type=jnp.float32)
    up = jnp.dot(a, w["w_up"], preferred_element_type=jnp.float32)
    return h + matmul((jax.nn.silu(gate) * up).astype(jnp.bfloat16), w["w_down"])


def stack(weights, h):
    return lax.scan(lambda h, w: (layer(h, w), None), h, weights)[0]


def reference(x, dy, w_gate, w_up, w_down):
    weights = dict(zip(NAMES, (w_gate, w_up, w_down), strict=True))

    def take(so_far, sequence):
        h, by_y = sequence
        _, back = jax.vjp(stack, weights, h)
        by_weights, by_h = back(by_y)
        return jax.tree.map(lambda total, term: total + term.astype(jnp.float32), so_far, by_weights), by_h

    none_yet = {name: jnp.zeros(w.shape, jnp.float32) for name, w in weights.items()}
    by_weights, by_x = lax.scan(take, none_yet, (x, dy))
    return (by_x, *(by_weights[name].astype(jnp.bfloat16) for name in NAMES))
```

```python
import functools

import jax
import jax.numpy as jnp
from jax import lax
from jax.experimental import pallas as pl
from jax.experimental.pallas import tpu as pltpu
from jax.sharding import PartitionSpec as P

BF, F32 = jnp.bfloat16, jnp.float32
MESH = pl.DeviceIdType.MESH
TB = 512


def pos(q):
    return (q % 2) * 2 + q // 2


def dot(a, b):
    return jnp.dot(a, b, preferred_element_type=F32)


def dot_t(a, b):
    return lax.dot_general(a, b, (((1,), (1,)), ((), ())), preferred_element_type=F32)


def kernel(NC, x_h, dy_h, wg_h, wu_h, wd_h,
           dx_o, og_o, ou_o, od_o, gxg, gxu, gxd, gdg, gdu, gdd, psg, psu, psd,
           hb, dyb, ab, aT, acc, WG, WU, WD, pT, dgb, dub,
           szg, szu, szd, rzg, rzu, rzd, Gg, Gu, Gd, sxg, sxu, sxd, rxg, rxu, rxd, obg, obu, obd,
           io_s, ld_s, ps_s, ps_r, ax_s, ax_r, ay_s, ay_r, az_s, az_r,
           z_s, z_r, x_s, x_r, o_s):
    T, D = ab.shape
    FC = dgb.shape[1]
    L = wg_h.shape[0]
    Q = wg_h.shape[1]
    S = FC // 4
    FD = wd_h.shape[1]
    Q2, S2 = Q // 2, S // 2
    NB = T // TB
    r = lax.axis_index("rep")
    me = lax.axis_index("dp")
    c, k = me // 2, me % 2
    xp = {"rep": r, "dp": (1 - c) * 2 + k}
    yp = {"rep": 1 - r, "dp": me}
    zp = {"rep": r, "dp": c * 2 + 1 - k}
    zq = c * 2 + 1 - k
    xq = (1 - c) * 2 + k
    dq = (1 - c) * 2 + 1 - k

    def m_of(i, n):
        return pl.multiple_of(i, n)

    def remote(src, dst, ss, rs, dev):
        return pltpu.make_async_remote_copy(src, dst, ss, rs, device_id=dev, device_id_type=MESH)

    def half(m, h):
        n = S2 if m == 2 else Q2
        return pl.ds(m_of(h * n, n), n)

    W_in = (wg_h, wu_h, wd_h)
    GX, GD, PS, WV = (gxg, gxu, gxd), (gdg, gdu, gdd), (psg, psu, psd), (WG, WU, WD)

    def strips(m, l, j, h=None):
        if m == 2:
            n = S if h is None else S2
            at = j * S if h is None else j * S + h * S2
            return [((l, pl.ds(m_of(at, n), n), slice(None)), None)]
        rows = slice(None) if h is None else half(m, h)
        return [((l, rows, pl.ds(m_of(d * FD + j * S, S), S)), pl.ds(pos(d) * S, S)) for d in range(4)]

    def send_x(s):
        l, j = s // NC, s % NC
        for m in range(3):
            for src, cols in strips(m, l, j, r):
                dst = GX[m].at[l, j, half(m, r)] if cols is None else GX[m].at[l, j, half(m, r), cols]
                remote(W_in[m].at[src], dst, ax_s.at[m, s], ax_r.at[m, s], xp).start()

    def send_ps(l):
        for m in range(3):
            remote(W_in[m].at[l], PS[m].at[l], ps_s.at[m, l], ps_r.at[m, l], zp).start()

    def whole(m, s, h, ss, rs, dev, G=None):
        l, j = s // NC, s % NC
        src = GX[m].at[l, j, half(m, h)]
        return remote(src, (G or GX)[m].at[l, j, half(m, h)], ss, rs, dev)

    def stage1(s):
        for m in range(3):
            whole(m, s, r, ax_s.at[m, s], ax_r.at[m, s], xp).wait_recv()
            whole(m, s, r, ay_s.at[m, s], ay_r.at[m, s], yp).start()
            whole(m, s, r, az_s.at[0, m, s], az_r.at[0, m, s], zp, GD).start()

    def stage2(s):
        for m in range(3):
            whole(m, s, 1 - r, ay_s.at[m, s], ay_r.at[m, s], yp).wait_recv()
            whole(m, s, 1 - r, az_s.at[1, m, s], az_r.at[1, m, s], zp, GD).start()

    def ready(s):
        for i in range(2):
            for m in range(3):
                whole(m, s, r if i == 0 else 1 - r, az_s.at[i, m, s], az_r.at[i, m, s], zp, GD).wait_recv()

        @pl.when(s % NC == 0)
        def _():
            l = s // NC
            for m in range(3):
                remote(W_in[m].at[l], PS[m].at[l], ps_s.at[m, l], ps_r.at[m, l], zp).wait_recv()

    def drain_ag():
        @pl.loop(0, L * NC)
        def _(s):
            for m in range(3):
                whole(m, s, r, ax_s.at[m, s], ax_r.at[m, s], xp).wait_send()
                whole(m, s, r, ay_s.at[m, s], ay_r.at[m, s], yp).wait_send()
                for i in range(2):
                    whole(m, s, r, az_s.at[i, m, s], az_r.at[i, m, s], zp, GD).wait_send()
        for l in range(L):
            for m in range(3):
                remote(W_in[m].at[l], PS[m].at[l], ps_s.at[m, l], ps_r.at[m, l], zp).wait_send()

    def load(step):
        l, j, slot = (step // NC) % 2, step % NC, step % 2
        for m in range(3):
            for q, src in ((me, W_in[m]), (zq, PS[m])):
                for at, cols in strips(m, l, j):
                    if m == 2:
                        dst = WV[m].at[slot, pl.ds(m_of(((q % 2) * 2 + q // 2) * S, S), S)]
                    else:
                        dst = WV[m].at[slot, pl.ds(m_of(q * Q, Q), Q), cols]
                    pltpu.make_async_copy(src.at[at], dst, ld_s.at[m, slot]).start()
            for q, src in ((xq, GX[m]), (dq, GD[m])):
                if m == 2:
                    dst = WV[m].at[slot, pl.ds(m_of(((q % 2) * 2 + q // 2) * S, S), S)]
                else:
                    dst = WV[m].at[slot, pl.ds(m_of(q * Q, Q), Q)]
                pltpu.make_async_copy(src.at[l, j], dst, ld_s.at[m, slot]).start()

    def loaded(step):
        slot = step % 2
        for m in range(3):
            pltpu.make_async_copy(WV[m].at[slot], WV[m].at[slot], ld_s.at[m, slot]).wait()

    SZ, RZ, G32, SX, RX, OB = (szg, szu, szd), (rzg, rzu, rzd), (Gg, Gu, Gd), (sxg, sxu, sxd), (rxg, rxu, rxd), (obg, obu, obd)
    HR = (2 * Q, 2 * Q, 2 * S)
    QR = (Q, Q, S)

    def to_z(m, s):
        return remote(SZ[m], RZ[m].at[s % 2], z_s.at[m], z_r.at[m, s % 2], zp)

    def to_x(m, s):
        return remote(SX[m].at[s % 2], RX[m].at[s % 4], x_s.at[m, s % 2], x_r.at[m, s % 4], xp)

    def grads(s, base, m):
        rows = pl.ds(m_of(base * HR[m], HR[m]), HR[m])
        if m == 2:
            return dot(pT[rows, :], dyb[...])
        return dot(aT[rows, :], (dgb, dub)[m][...])

    def produce(s):
        for m in (2, 0, 1):
            SZ[m][...] = grads(s, 1 - k, m).astype(BF)
            to_z(m, s).start()
        for m in (2, 0, 1):
            G32[m][s % 2] = grads(s, k, m)

    def reduce_x(s):
        for m in (2, 0, 1):
            @pl.when(s >= 2)
            def _():
                to_x(m, s).wait_send()
            to_z(m, s).wait()
            mine, other = pl.ds(m_of(c * QR[m], QR[m]), QR[m]), pl.ds(m_of((1 - c) * QR[m], QR[m]), QR[m])
            SX[m][s % 2] = (G32[m][s % 2, other] + RZ[m][s % 2, other].astype(F32)).astype(BF)
            to_x(m, s).start()
            G32[m][s % 2, mine] += RZ[m][s % 2, mine].astype(F32)

    def out_copies(s):
        l, j = 1 - s // NC, s % NC
        for m in range(3):
            for at, cols in strips(m, l, j):
                src = OB[m].at[s % 2] if cols is None else OB[m].at[s % 2, :, cols]
                yield pltpu.make_async_copy(src, (og_o, ou_o, od_o)[m].at[at], o_s.at[m, s % 2])

    def out_wait(s):
        for m in range(3):
            pltpu.make_async_copy(OB[m].at[s % 2], OB[m].at[s % 2], o_s.at[m, s % 2]).wait()

    def finish(s):
        @pl.when(s >= 2)
        def _():
            out_wait(s)
        for m in (2, 0, 1):
            to_x(m, s).wait_recv()
            mine = pl.ds(m_of(c * QR[m], QR[m]), QR[m])
            OB[m][s % 2] = (G32[m][s % 2, mine] + RX[m][s % 4].astype(F32)).astype(BF)
        for copy in out_copies(s):
            copy.start()

    def scale_of(wide):
        return lax.rsqrt(jnp.mean(wide * wide, -1, keepdims=True) + 1e-6)

    def norm(l, transposed):
        @pl.loop(0, T // 256)
        def _(t):
            rows = pl.ds(m_of(t * 256, 256), 256)
            wide = hb[l, rows, :].astype(F32)
            a = (wide * scale_of(wide)).astype(BF)
            ab[rows, :] = a
            acc[rows, :] = jnp.zeros((256, D), F32)
            if transposed:
                at = a.T
                for q in range(4):
                    aT[pl.ds(pos(q) * Q, Q), rows] = at[q * Q:(q + 1) * Q]

    def fwd_block(slot, t):
        rows = pl.ds(m_of(t * TB, TB), TB)
        a = ab[rows, :]
        ps = []
        for n in range(0, FC, 256):
            g = dot(a, WG[slot, :, n:n + 256])
            u = dot(a, WU[slot, :, n:n + 256])
            p = (g * (1.0 / (1.0 + jnp.exp(-g))) * u).astype(BF)
            ps.append(p)
        acc[rows, :] += dot(jnp.concatenate(ps, 1), WD[slot])

    def bwd_block(slot, t):
        rows = pl.ds(m_of(t * TB, TB), TB)
        a = ab[rows, :]
        dy = dyb[rows, :]
        for n in range(0, FC, 256):
            g = dot(a, WG[slot, :, n:n + 256])
            u = dot(a, WU[slot, :, n:n + 256])
            dp = dot_t(dy, WD[slot, n:n + 256, :]).astype(BF).astype(F32)
            sig = 1.0 / (1.0 + jnp.exp(-g))
            silu = g * sig
            p = (silu * u).astype(BF)
            pT[n:n + 256, rows] = p.T
            dub[rows, n:n + 256] = (dp * silu).astype(BF)
            dgb[rows, n:n + 256] = (dp * u * (sig * (1.0 + g * (1.0 - sig)))).astype(BF)
        acc[rows, :] += dot_t(dgb[rows, :], WG[slot]) + dot_t(dub[rows, :], WU[slot])

    def norm_back(l):
        @pl.loop(0, T // 256)
        def _(t):
            rows = pl.ds(m_of(t * 256, 256), 256)
            wide = hb[l, rows, :].astype(F32)
            sc = scale_of(wide)
            da = acc[rows, :].astype(BF).astype(F32)
            inner = jnp.sum(da * wide, -1, keepdims=True)
            dh = da * sc - wide * (sc * sc * sc * inner * (1.0 / D))
            dyb[rows, :] = (dyb[rows, :].astype(F32) + dh.astype(BF).astype(F32)).astype(BF)

    in_x = pltpu.make_async_copy(x_h, hb.at[0], io_s.at[0])
    in_dy = pltpu.make_async_copy(dy_h, dyb, io_s.at[1])
    in_x.start()
    in_dy.start()
    barrier = pltpu.get_barrier_semaphore()
    for dev in (xp, yp, zp):
        pl.semaphore_signal(barrier, inc=1, device_id=dev, device_id_type=MESH)
    pl.semaphore_wait(barrier, 3)
    send_x(0)
    send_ps(0)

    @pl.loop(1, NC)
    def _(s):
        send_x(s)
    in_x.wait()
    norm(0, False)
    in_dy.wait()
    stage1(0)
    stage1(1)
    stage2(0)
    ready(0)
    load(0)

    @pl.loop(0, NC)
    def _(j):
        loaded(j)
        send_x(NC + j)

        @pl.when(j == 0)
        def _():
            send_ps(1)

        @pl.loop(0, NB)
        def _(t):
            fwd_block(j % 2, t)

            @pl.when(t == 0)
            def _():
                stage1(j + 2)

            @pl.when(t == 1)
            def _():
                stage2(j + 1)

            @pl.when(t == 2)
            def _():
                ready(j + 1)
                load(j + 1)

    @pl.loop(0, T // 256)
    def _(t):
        rows = pl.ds(m_of(t * 256, 256), 256)
        hb[1, rows, :] = (hb[0, rows, :].astype(F32) + acc[rows, :].astype(BF).astype(F32)).astype(BF)

    @pl.loop(0, 2)
    def _(phase):
        norm(1 - phase, True)

        @pl.loop(0, NC)
        def _(j):
            s = phase * NC + j
            step = NC + s
            loaded(step)

            @pl.loop(0, NB)
            def _(t):
                bwd_block(step % 2, t)

                @pl.when(t == 0)
                def _():
                    @pl.when(s >= 1)
                    def _():
                        reduce_x(s - 1)

                    @pl.when(step + 2 < 2 * NC)
                    def _():
                        stage1(step + 2)

                @pl.when(t == 1)
                def _():
                    @pl.when(step + 1 < 2 * NC)
                    def _():
                        stage2(step + 1)

                @pl.when(t == 2)
                def _():
                    @pl.when(s >= 2)
                    def _():
                        finish(s - 2)

                    @pl.when(step + 1 < 2 * NC)
                    def _():
                        ready(step + 1)

                    @pl.when(step + 1 < 3 * NC)
                    def _():
                        load(step + 1)
            produce(s)
        norm_back(1 - phase)

    last = 2 * NC - 1
    out_dx = pltpu.make_async_copy(dyb, dx_o, io_s.at[0])
    out_dx.start()
    reduce_x(last)
    finish(last - 1)
    drain_ag()
    finish(last)
    for s in (last - 1, last):
        for m in range(3):
            to_x(m, s).wait_send()
        out_wait(s)
    out_dx.wait()


def solution(mesh):
    def local(x, dy, wg, wu, wd):
        _, T, D = x.shape
        L, Q, F = wg.shape
        FD = wd.shape[1]
        NC = 6
        FC = F // NC
        S = FC // 4
        sds = jax.ShapeDtypeStruct
        hbm = pl.BlockSpec(memory_space=pltpu.HBM)
        V, DMA = pltpu.VMEM, pltpu.SemaphoreType.DMA
        gate, down = (L, NC, Q, FC), (L, NC, S, D)
        outs = [sds((T, D), BF), sds(wg.shape, BF), sds(wu.shape, BF), sds(wd.shape, BF)]
        outs += [sds(s, BF) for s in (gate, gate, down) * 2]
        outs += [sds(t.shape, BF) for t in (wg, wu, wd)]
        scratch = [V((2, T, D), BF), V((T, D), BF), V((T, D), BF), V((D, T), BF), V((T, D), F32),
                   V((2, D, FC), BF), V((2, D, FC), BF), V((2, FC, D), BF),
                   V((FC, T), BF), V((T, FC), BF), V((T, FC), BF)]
        h3 = ((2 * Q, FC), (2 * Q, FC), (2 * S, D))
        q3 = ((Q, FC), (Q, FC), (S, D))
        scratch += [V(s, BF) for s in h3] + [V((2, *s), BF) for s in h3] + [V((2, *s), F32) for s in h3]
        scratch += [V((2, *s), BF) for s in q3] + [V((4, *s), BF) for s in q3] + [V((2, *s), BF) for s in q3]
        LC = L * NC
        scratch += [DMA((2,)), DMA((3, 2)), DMA((3, L)), DMA((3, L)), DMA((3, LC)), DMA((3, LC)), DMA((3, LC)), DMA((3, LC)),
                    DMA((2, 3, LC)), DMA((2, 3, LC)), DMA((3,)), DMA((3, 2)), DMA((3, 2)), DMA((3, 4)), DMA((3, 2))]
        res = pl.pallas_call(
            functools.partial(kernel, NC),
            out_shape=outs,
            in_specs=[hbm] * 5,
            out_specs=[hbm] * len(outs),
            scratch_shapes=scratch,
            compiler_params=pltpu.CompilerParams(collective_id=0, has_side_effects=True, vmem_limit_bytes=67043328),
        )(x[0], dy[0], wg, wu, wd)
        return (res[0][None], *res[1:4])

    seq, w = P(("rep", "dp"), None, None), P(None, "dp", None)
    grad = P("rep", "dp", None)
    return jax.shard_map(local, mesh=mesh, in_specs=(seq, seq, w, w, w), out_specs=(seq, grad, grad, grad), check_vma=False)
```

```python
import functools

import jax
import jax.numpy as jnp
from jax import lax
from jax.experimental import pallas as pl
from jax.experimental.pallas import tpu as pltpu
from jax.sharding import PartitionSpec as P

BF, F32 = jnp.bfloat16, jnp.float32
MESH = pl.DeviceIdType.MESH
TB = 512


def pos(q):
    return (q % 2) * 2 + q // 2


def dot(a, b):
    return jnp.dot(a, b, preferred_element_type=F32)


def dot_t(a, b):
    return lax.dot_general(a, b, (((1,), (1,)), ((), ())), preferred_element_type=F32)


def kernel(NC, x_h, dy_h, wg_h, wu_h, wd_h,
           dx_o, og_o, ou_o, od_o, gxg, gxu, gxd, gdg, gdu, gdd, psg, psu, psd, g_h, u_h,
           hb, dyb, ab, aT, acc, WG, WU, WD, pT, dgb, dub, gst, ust, gu_s,
           szg, szu, szd, rzg, rzu, rzd, Gg, Gu, Gd, sxg, sxu, sxd, rxg, rxu, rxd, obg, obu, obd,
           io_s, ld_s, ps_s, ps_r, ax_s, ax_r, ay_s, ay_r, az_s, az_r,
           z_s, z_r, x_s, x_r, o_s):
    T, D = ab.shape
    FC = dgb.shape[1]
    L = wg_h.shape[0]
    Q = wg_h.shape[1]
    S = FC // 4
    FD = wd_h.shape[1]
    Q2, S2 = Q // 2, S // 2
    NB = T // TB
    r = lax.axis_index("rep")
    me = lax.axis_index("dp")
    c, k = me // 2, me % 2
    xp = {"rep": r, "dp": (1 - c) * 2 + k}
    yp = {"rep": 1 - r, "dp": me}
    zp = {"rep": r, "dp": c * 2 + 1 - k}
    zq = c * 2 + 1 - k
    xq = (1 - c) * 2 + k
    dq = (1 - c) * 2 + 1 - k

    def m_of(i, n):
        return pl.multiple_of(i, n)

    def remote(src, dst, ss, rs, dev):
        return pltpu.make_async_remote_copy(src, dst, ss, rs, device_id=dev, device_id_type=MESH)

    def half(m, h):
        n = S2 if m == 2 else Q2
        return pl.ds(m_of(h * n, n), n)

    W_in = (wg_h, wu_h, wd_h)
    GX, GD, PS, WV = (gxg, gxu, gxd), (gdg, gdu, gdd), (psg, psu, psd), (WG, WU, WD)

    def strips(m, l, j, h=None):
        if m == 2:
            n = S if h is None else S2
            at = j * S if h is None else j * S + h * S2
            return [((l, pl.ds(m_of(at, n), n), slice(None)), None)]
        rows = slice(None) if h is None else half(m, h)
        return [((l, rows, pl.ds(m_of(d * FD + j * S, S), S)), pl.ds(pos(d) * S, S)) for d in range(4)]

    def send_x(s):
        l, j = s // NC, s % NC
        for m in range(3):
            for src, cols in strips(m, l, j, r):
                dst = GX[m].at[l, j, half(m, r)] if cols is None else GX[m].at[l, j, half(m, r), cols]
                remote(W_in[m].at[src], dst, ax_s.at[m, s], ax_r.at[m, s], xp).start()

    def send_ps(l):
        for m in range(3):
            remote(W_in[m].at[l], PS[m].at[l], ps_s.at[m, l], ps_r.at[m, l], zp).start()

    def whole(m, s, h, ss, rs, dev, G=None):
        l, j = s // NC, s % NC
        src = GX[m].at[l, j, half(m, h)]
        return remote(src, (G or GX)[m].at[l, j, half(m, h)], ss, rs, dev)

    def stage1(s):
        for m in range(3):
            whole(m, s, r, ax_s.at[m, s], ax_r.at[m, s], xp).wait_recv()
            whole(m, s, r, ay_s.at[m, s], ay_r.at[m, s], yp).start()
            whole(m, s, r, az_s.at[0, m, s], az_r.at[0, m, s], zp, GD).start()

    def stage2(s):
        for m in range(3):
            whole(m, s, 1 - r, ay_s.at[m, s], ay_r.at[m, s], yp).wait_recv()
            whole(m, s, 1 - r, az_s.at[1, m, s], az_r.at[1, m, s], zp, GD).start()

    def ready(s):
        for i in range(2):
            for m in range(3):
                whole(m, s, r if i == 0 else 1 - r, az_s.at[i, m, s], az_r.at[i, m, s], zp, GD).wait_recv()

        @pl.when(s % NC == 0)
        def _():
            l = s // NC
            for m in range(3):
                remote(W_in[m].at[l], PS[m].at[l], ps_s.at[m, l], ps_r.at[m, l], zp).wait_recv()

    def drain_ag():
        @pl.loop(0, L * NC)
        def _(s):
            for m in range(3):
                whole(m, s, r, ax_s.at[m, s], ax_r.at[m, s], xp).wait_send()
                whole(m, s, r, ay_s.at[m, s], ay_r.at[m, s], yp).wait_send()
                for i in range(2):
                    whole(m, s, r, az_s.at[i, m, s], az_r.at[i, m, s], zp, GD).wait_send()
        for l in range(L):
            for m in range(3):
                remote(W_in[m].at[l], PS[m].at[l], ps_s.at[m, l], ps_r.at[m, l], zp).wait_send()

    def load(step):
        l, j, slot = (step // NC) % 2, step % NC, step % 2
        for m in range(3):
            for q, src in ((me, W_in[m]), (zq, PS[m])):
                for at, cols in strips(m, l, j):
                    if m == 2:
                        dst = WV[m].at[slot, pl.ds(m_of(((q % 2) * 2 + q // 2) * S, S), S)]
                    else:
                        dst = WV[m].at[slot, pl.ds(m_of(q * Q, Q), Q), cols]
                    pltpu.make_async_copy(src.at[at], dst, ld_s.at[m, slot]).start()
            for q, src in ((xq, GX[m]), (dq, GD[m])):
                if m == 2:
                    dst = WV[m].at[slot, pl.ds(m_of(((q % 2) * 2 + q // 2) * S, S), S)]
                else:
                    dst = WV[m].at[slot, pl.ds(m_of(q * Q, Q), Q)]
                pltpu.make_async_copy(src.at[l, j], dst, ld_s.at[m, slot]).start()

    def loaded(step):
        slot = step % 2
        for m in range(3):
            pltpu.make_async_copy(WV[m].at[slot], WV[m].at[slot], ld_s.at[m, slot]).wait()

    SZ, RZ, G32, SX, RX, OB = (szg, szu, szd), (rzg, rzu, rzd), (Gg, Gu, Gd), (sxg, sxu, sxd), (rxg, rxu, rxd), (obg, obu, obd)
    HR = (2 * Q, 2 * Q, 2 * S)
    QR = (Q, Q, S)

    def to_z(m, s):
        return remote(SZ[m], RZ[m].at[s % 2], z_s.at[m], z_r.at[m, s % 2], zp)

    def to_x(m, s):
        return remote(SX[m].at[s % 2], RX[m].at[s % 4], x_s.at[m, s % 2], x_r.at[m, s % 4], xp)

    def grads(m, part, n):
        rows = pl.ds(m_of(part * HR[m], HR[m]), HR[m])
        if m == 2:
            return dot(pT[rows, :], dyb[:, n:n + 256])
        return dot(aT[rows, :], (dgb, dub)[m][:, n:n + 256])

    def produce(s):
        slot = s % 2
        for n in range(0, D, 256):
            szd[:, n:n + 256] = grads(2, 1 - k, n).astype(BF)
            Gd[slot, :, n:n + 256] = grads(2, k, n)
        for m in (0, 1):
            for n in range(0, FC, 256):
                SZ[m][:, n:n + 256] = grads(m, 1 - k, n).astype(BF)
        for m in (2, 0, 1):
            to_z(m, s).start()
        for m in (0, 1):
            for n in range(0, FC, 256):
                G32[m][slot, :, n:n + 256] = grads(m, k, n)

    def reduce_x(s):
        for m in (2, 0, 1):
            @pl.when(s >= 2)
            def _():
                to_x(m, s).wait_send()
            to_z(m, s).wait()
            mine, other = pl.ds(m_of(c * QR[m], QR[m]), QR[m]), pl.ds(m_of((1 - c) * QR[m], QR[m]), QR[m])
            SX[m][s % 2] = (G32[m][s % 2, other] + RZ[m][s % 2, other].astype(F32)).astype(BF)
            to_x(m, s).start()
            G32[m][s % 2, mine] += RZ[m][s % 2, mine].astype(F32)

    def out_copies(s):
        l, j = 1 - s // NC, s % NC
        for m in range(3):
            for at, cols in strips(m, l, j):
                src = OB[m].at[s % 2] if cols is None else OB[m].at[s % 2, :, cols]
                yield pltpu.make_async_copy(src, (og_o, ou_o, od_o)[m].at[at], o_s.at[m, s % 2])

    def out_wait(s):
        for m in range(3):
            pltpu.make_async_copy(OB[m].at[s % 2], OB[m].at[s % 2], o_s.at[m, s % 2]).wait()

    def finish(s):
        @pl.when(s >= 2)
        def _():
            out_wait(s)
        for m in (2, 0, 1):
            to_x(m, s).wait_recv()
            mine = pl.ds(m_of(c * QR[m], QR[m]), QR[m])
            OB[m][s % 2] = (G32[m][s % 2, mine] + RX[m][s % 4].astype(F32)).astype(BF)
        for copy in out_copies(s):
            copy.start()

    def scale_of(wide):
        return lax.rsqrt(jnp.mean(wide * wide, -1, keepdims=True) + 1e-6)

    def norm(l, transposed):
        @pl.loop(0, T // 256)
        def _(t):
            rows = pl.ds(m_of(t * 256, 256), 256)
            wide = hb[l, rows, :].astype(F32)
            a = (wide * scale_of(wide)).astype(BF)
            ab[rows, :] = a
            acc[rows, :] = jnp.zeros((256, D), F32)
            if transposed:
                at = a.T
                for q in range(4):
                    aT[pl.ds(pos(q) * Q, Q), rows] = at[q * Q:(q + 1) * Q]

    def gu_copies(j, t, out):
        rows = pl.ds(m_of(t * TB, TB), TB)
        for i, (v, h) in enumerate(((gst, g_h), (ust, u_h))):
            pair = (v.at[t % 2], h.at[j, rows, :])
            yield pltpu.make_async_copy(*(pair if out else pair[::-1]), gu_s.at[i, t % 2])

    def fwd_block(slot, j, t):
        rows = pl.ds(t * TB, TB)
        a = ab[rows, :]
        ps = []
        for n in range(0, FC, 256):
            g = dot(a, WG[slot, :, n:n + 256])
            u = dot(a, WU[slot, :, n:n + 256])
            gst[t % 2, :, n:n + 256] = g
            ust[t % 2, :, n:n + 256] = u
            ps.append((g * (1.0 / (1.0 + jnp.exp(-g))) * u).astype(BF))
        p = jnp.concatenate(ps, 1)
        for n in range(0, D, 256):
            acc[rows, n:n + 256] += dot(p, WD[slot, :, n:n + 256])

    def bwd_ab(slot, t, saved):
        rows = pl.ds(t * TB, TB)
        a = None if saved else ab[rows, :]
        dy = dyb[rows, :]
        for n in range(0, FC, 256):
            dp = dot_t(dy, WD[slot, n:n + 256, :]).astype(BF).astype(F32)
            if saved:
                g, u = gst[t % 2, :, n:n + 256], ust[t % 2, :, n:n + 256]
            else:
                g = dot(a, WG[slot, :, n:n + 256])
                u = dot(a, WU[slot, :, n:n + 256])
            sig = 1.0 / (1.0 + jnp.exp(-g))
            silu = g * sig
            p = (silu * u).astype(BF)
            pT[n:n + 256, rows] = p.T
            dub[rows, n:n + 256] = (dp * silu).astype(BF)
            dgb[rows, n:n + 256] = (dp * u * (sig * (1.0 + g * (1.0 - sig)))).astype(BF)

    def bwd_c(slot, t):
        for i in range(2):
            rows = pl.ds(t * TB + i * TB // 2, TB // 2)
            for n in range(0, D, 256):
                acc[rows, n:n + 256] += dot_t(dgb[rows, :], WG[slot, n:n + 256, :]) + dot_t(dub[rows, :], WU[slot, n:n + 256, :])

    def norm_back(l):
        @pl.loop(0, T // 256)
        def _(t):
            rows = pl.ds(m_of(t * 256, 256), 256)
            wide = hb[l, rows, :].astype(F32)
            sc = scale_of(wide)
            da = acc[rows, :].astype(BF).astype(F32)
            inner = jnp.sum(da * wide, -1, keepdims=True)
            dh = da * sc - wide * (sc * sc * sc * inner * (1.0 / D))
            dyb[rows, :] = (dyb[rows, :].astype(F32) + dh.astype(BF).astype(F32)).astype(BF)

    in_x = pltpu.make_async_copy(x_h, hb.at[0], io_s.at[0])
    in_dy = pltpu.make_async_copy(dy_h, dyb, io_s.at[1])
    in_x.start()
    in_dy.start()
    barrier = pltpu.get_barrier_semaphore()
    for dev in (xp, yp, zp):
        pl.semaphore_signal(barrier, inc=1, device_id=dev, device_id_type=MESH)
    pl.semaphore_wait(barrier, 3)
    send_x(0)
    send_ps(0)

    @pl.loop(1, NC)
    def _(s):
        send_x(s)
    in_x.wait()
    norm(0, False)
    in_dy.wait()
    stage1(0)
    stage1(1)
    stage2(0)
    ready(0)
    load(0)

    @pl.loop(0, NC)
    def _(j):
        loaded(j)
        send_x(NC + j)

        @pl.when(j == 0)
        def _():
            send_ps(1)

        for t in range(NB):
            if t >= 2:
                for copy in gu_copies(j, t - 2, True):
                    copy.wait()
            else:
                @pl.when(j > 0)
                def _():
                    for copy in gu_copies(j - 1, t + NB - 2, True):
                        copy.wait()
            fwd_block(j % 2, j, t)
            for copy in gu_copies(j, t, True):
                copy.start()
            if t == 0:
                stage1(j + 2)
            if t == 1:
                stage2(j + 1)
            if t == 2:
                ready(j + 1)
                load(j + 1)

    for t in (NB - 2, NB - 1):
        for copy in gu_copies(NC - 1, t, True):
            copy.wait()

    @pl.loop(0, T // 256)
    def _(t):
        rows = pl.ds(m_of(t * 256, 256), 256)
        hb[1, rows, :] = (hb[0, rows, :].astype(F32) + acc[rows, :].astype(BF).astype(F32)).astype(BF)

    for phase in range(2):
        norm(1 - phase, True)
        if phase == 1:
            for t in range(2):
                for copy in gu_copies(0, t, False):
                    copy.start()

        @pl.loop(0, NC)
        def _(j):
            s = phase * NC + j
            step = NC + s
            slot = step % 2
            loaded(step)

            def ab_of(t):
                if phase == 1:
                    for copy in gu_copies(j, t, False):
                        copy.wait()
                bwd_ab(slot, t, phase == 1)
                if phase == 1:
                    if t + 2 < NB:
                        for copy in gu_copies(j, t + 2, False):
                            copy.start()
                    else:
                        @pl.when(j + 1 < NC)
                        def _():
                            for copy in gu_copies(j + 1, t + 2 - NB, False):
                                copy.start()

            ab_of(0)

            @pl.when(s >= 1)
            def _():
                reduce_x(s - 1)

            @pl.when(step + 2 < 2 * NC)
            def _():
                stage1(step + 2)

            bwd_c(slot, 0)
            ab_of(1)
            bwd_c(slot, 1)
            ab_of(2)

            @pl.when(step + 1 < 2 * NC)
            def _():
                stage2(step + 1)

            @pl.when(s >= 2)
            def _():
                finish(s - 2)

            @pl.when(step + 1 < 2 * NC)
            def _():
                ready(step + 1)

            @pl.when(step + 1 < 3 * NC)
            def _():
                load(step + 1)

            bwd_c(slot, 2)
            ab_of(3)
            bwd_c(slot, 3)
            produce(s)
        norm_back(1 - phase)

    last = 2 * NC - 1
    out_dx = pltpu.make_async_copy(dyb, dx_o, io_s.at[0])
    out_dx.start()
    reduce_x(last)
    finish(last - 1)
    drain_ag()
    finish(last)
    for s in (last - 1, last):
        for m in range(3):
            to_x(m, s).wait_send()
        out_wait(s)
    out_dx.wait()


def solution(mesh):
    def local(x, dy, wg, wu, wd):
        _, T, D = x.shape
        L, Q, F = wg.shape
        FD = wd.shape[1]
        NC = 6
        FC = F // NC
        S = FC // 4
        sds = jax.ShapeDtypeStruct
        hbm = pl.BlockSpec(memory_space=pltpu.HBM)
        V, DMA = pltpu.VMEM, pltpu.SemaphoreType.DMA
        gate, down = (L, NC, Q, FC), (L, NC, S, D)
        outs = [sds((T, D), BF), sds(wg.shape, BF), sds(wu.shape, BF), sds(wd.shape, BF)]
        outs += [sds(s, BF) for s in (gate, gate, down) * 2]
        outs += [sds(t.shape, BF) for t in (wg, wu, wd)]
        outs += [sds((NC, T, FC), F32)] * 2
        scratch = [V((2, T, D), BF), V((T, D), BF), V((T, D), BF), V((D, T), BF), V((T, D), F32),
                   V((2, D, FC), BF), V((2, D, FC), BF), V((2, FC, D), BF),
                   V((FC, T), BF), V((T, FC), BF), V((T, FC), BF),
                   V((2, TB, FC), F32), V((2, TB, FC), F32), DMA((2, 2))]
        h3 = ((2 * Q, FC), (2 * Q, FC), (2 * S, D))
        q3 = ((Q, FC), (Q, FC), (S, D))
        scratch += [V(s, BF) for s in h3] + [V((2, *s), BF) for s in h3] + [V((2, *s), F32) for s in h3]
        scratch += [V((2, *s), BF) for s in q3] + [V((4, *s), BF) for s in q3] + [V((2, *s), BF) for s in q3]
        LC = L * NC
        scratch += [DMA((2,)), DMA((3, 2)), DMA((3, L)), DMA((3, L)), DMA((3, LC)), DMA((3, LC)), DMA((3, LC)), DMA((3, LC)),
                    DMA((2, 3, LC)), DMA((2, 3, LC)), DMA((3,)), DMA((3, 2)), DMA((3, 2)), DMA((3, 4)), DMA((3, 2))]
        res = pl.pallas_call(
            functools.partial(kernel, NC),
            out_shape=outs,
            in_specs=[hbm] * 5,
            out_specs=[hbm] * len(outs),
            scratch_shapes=scratch,
            compiler_params=pltpu.CompilerParams(collective_id=0, has_side_effects=True, vmem_limit_bytes=67043328),
        )(x[0], dy[0], wg, wu, wd)
        return (res[0][None], *res[1:4])

    seq, w = P(("rep", "dp"), None, None), P(None, "dp", None)
    grad = P("rep", "dp", None)
    return jax.shard_map(local, mesh=mesh, in_specs=(seq, seq, w, w, w), out_specs=(seq, grad, grad, grad), check_vma=False)
```

```python
import functools

import jax
import jax.numpy as jnp
from jax import lax
from jax.experimental import pallas as pl
from jax.experimental.pallas import tpu as pltpu
from jax.sharding import PartitionSpec as P

BF, F32 = jnp.bfloat16, jnp.float32
MESH = pl.DeviceIdType.MESH
TB = 512


def pos(q):
    return (q % 2) * 2 + q // 2


def dot(a, b):
    return jnp.dot(a, b, preferred_element_type=F32)


def dot_t(a, b):
    return lax.dot_general(a, b, (((1,), (1,)), ((), ())), preferred_element_type=F32)


def kernel(NC, x_h, dy_h, wg_h, wu_h, wd_h,
           dx_o, og_o, ou_o, od_o, gxg, gxu, gxd, gdg, gdu, gdd, psg, psu, psd, g_h, u_h,
           hb, dyb, ab, aT, acc, WG, WU, WD, pT, dgb, dub, gst, ust, gu_s,
           szg, szu, szd, rzg, rzu, rzd, Gg, Gu, Gd, sxg, sxu, sxd, rxg, rxu, rxd, obg, obu, obd,
           io_s, ld_s, ps_s, ps_r, ax_s, ax_r, ay_s, ay_r, az_s, az_r,
           z_s, z_r, x_s, x_r, o_s):
    T, D = ab.shape
    FC = dgb.shape[1]
    L = wg_h.shape[0]
    Q = wg_h.shape[1]
    S = FC // 4
    FD = wd_h.shape[1]
    Q2, S2 = Q // 2, S // 2
    NB = T // TB
    r = lax.axis_index("rep")
    me = lax.axis_index("dp")
    c, k = me // 2, me % 2
    xp = {"rep": r, "dp": (1 - c) * 2 + k}
    yp = {"rep": 1 - r, "dp": me}
    zp = {"rep": r, "dp": c * 2 + 1 - k}
    zq = c * 2 + 1 - k
    xq = (1 - c) * 2 + k
    dq = (1 - c) * 2 + 1 - k

    def m_of(i, n):
        return pl.multiple_of(i, n)

    def remote(src, dst, ss, rs, dev):
        return pltpu.make_async_remote_copy(src, dst, ss, rs, device_id=dev, device_id_type=MESH)

    def half(m, h):
        n = S2 if m == 2 else Q2
        return pl.ds(m_of(h * n, n), n)

    W_in = (wg_h, wu_h, wd_h)
    GX, GD, PS, WV = (gxg, gxu, gxd), (gdg, gdu, gdd), (psg, psu, psd), (WG, WU, WD)

    def strips(m, l, j, h=None):
        if m == 2:
            n = S if h is None else S2
            at = j * S if h is None else j * S + h * S2
            return [((l, pl.ds(m_of(at, n), n), slice(None)), None)]
        rows = slice(None) if h is None else half(m, h)
        return [((l, rows, pl.ds(m_of(d * FD + j * S, S), S)), pl.ds(pos(d) * S, S)) for d in range(4)]

    def send_x(s):
        l, j = s // NC, s % NC
        for m in range(3):
            for src, cols in strips(m, l, j, r):
                dst = GX[m].at[l, j, half(m, r)] if cols is None else GX[m].at[l, j, half(m, r), cols]
                remote(W_in[m].at[src], dst, ax_s.at[m, s], ax_r.at[m, s], xp).start()

    def send_ps(l):
        for m in range(3):
            remote(W_in[m].at[l], PS[m].at[l], ps_s.at[m, l], ps_r.at[m, l], zp).start()

    def whole(m, s, h, ss, rs, dev, G=None):
        l, j = s // NC, s % NC
        src = GX[m].at[l, j, half(m, h)]
        return remote(src, (G or GX)[m].at[l, j, half(m, h)], ss, rs, dev)

    def stage1(s):
        for m in range(3):
            whole(m, s, r, ax_s.at[m, s], ax_r.at[m, s], xp).wait_recv()
            whole(m, s, r, ay_s.at[m, s], ay_r.at[m, s], yp).start()
            whole(m, s, r, az_s.at[0, m, s], az_r.at[0, m, s], zp, GD).start()

    def stage2(s):
        for m in range(3):
            whole(m, s, 1 - r, ay_s.at[m, s], ay_r.at[m, s], yp).wait_recv()
            whole(m, s, 1 - r, az_s.at[1, m, s], az_r.at[1, m, s], zp, GD).start()

    def ready(s):
        for i in range(2):
            for m in range(3):
                whole(m, s, r if i == 0 else 1 - r, az_s.at[i, m, s], az_r.at[i, m, s], zp, GD).wait_recv()

        @pl.when(s % NC == 0)
        def _():
            l = s // NC
            for m in range(3):
                remote(W_in[m].at[l], PS[m].at[l], ps_s.at[m, l], ps_r.at[m, l], zp).wait_recv()

    def drain_ag():
        @pl.loop(0, L * NC)
        def _(s):
            for m in range(3):
                whole(m, s, r, ax_s.at[m, s], ax_r.at[m, s], xp).wait_send()
                whole(m, s, r, ay_s.at[m, s], ay_r.at[m, s], yp).wait_send()
                for i in range(2):
                    whole(m, s, r, az_s.at[i, m, s], az_r.at[i, m, s], zp, GD).wait_send()
        for l in range(L):
            for m in range(3):
                remote(W_in[m].at[l], PS[m].at[l], ps_s.at[m, l], ps_r.at[m, l], zp).wait_send()

    def load(step):
        l, j, slot = (step // NC) % 2, step % NC, step % 2
        for m in range(3):
            for q, src in ((me, W_in[m]), (zq, PS[m])):
                for at, cols in strips(m, l, j):
                    if m == 2:
                        dst = WV[m].at[slot, pl.ds(m_of(((q % 2) * 2 + q // 2) * S, S), S)]
                    else:
                        dst = WV[m].at[slot, pl.ds(m_of(q * Q, Q), Q), cols]
                    pltpu.make_async_copy(src.at[at], dst, ld_s.at[m, slot]).start()
            for q, src in ((xq, GX[m]), (dq, GD[m])):
                if m == 2:
                    dst = WV[m].at[slot, pl.ds(m_of(((q % 2) * 2 + q // 2) * S, S), S)]
                else:
                    dst = WV[m].at[slot, pl.ds(m_of(q * Q, Q), Q)]
                pltpu.make_async_copy(src.at[l, j], dst, ld_s.at[m, slot]).start()

    def loaded(step):
        slot = step % 2
        for m in range(3):
            pltpu.make_async_copy(WV[m].at[slot], WV[m].at[slot], ld_s.at[m, slot]).wait()

    SZ, RZ, G32, SX, RX, OB = (szg, szu, szd), (rzg, rzu, rzd), (Gg, Gu, Gd), (sxg, sxu, sxd), (rxg, rxu, rxd), (obg, obu, obd)
    HR = (2 * Q, 2 * Q, 2 * S)
    QR = (Q, Q, S)

    def to_z(m, s):
        return remote(SZ[m], RZ[m].at[s % 2], z_s.at[m], z_r.at[m, s % 2], zp)

    def to_x(m, s):
        return remote(SX[m].at[s % 2], RX[m].at[s % 4], x_s.at[m, s % 2], x_r.at[m, s % 4], xp)

    def grads(m, part, n, l=0):
        rows = pl.ds(m_of(part * HR[m], HR[m]), HR[m])
        if m == 2:
            return dot(pT[rows, :], dyb[:, n:n + 256])
        return dot(aT[l, rows, :], (dgb, dub)[m][:, n:n + 256])

    def grads_first(slot, l):
        for n in range(0, D, 256):
            szd[:, n:n + 256] = grads(2, 1 - k, n).astype(BF)
            Gd[slot, :, n:n + 256] = grads(2, k, n)
        for m in (0, 1):
            for n in range(0, FC, 256):
                SZ[m][:, n:n + 256] = grads(m, 1 - k, n, l).astype(BF)

    def grads_mine(slot, l):
        for m in (0, 1):
            for n in range(0, FC, 256):
                G32[m][slot, :, n:n + 256] = grads(m, k, n, l)

    def chip_wait(ms, s):
        for m in ms:
            @pl.when(s >= 2)
            def _():
                to_x(m, s).wait_send()
            to_z(m, s).wait()

    def chip_sum(ms, slot):
        for m in ms:
            mine, other = pl.ds(m_of(c * QR[m], QR[m]), QR[m]), pl.ds(m_of((1 - c) * QR[m], QR[m]), QR[m])
            SX[m][slot] = (G32[m][slot, other] + RZ[m][slot, other].astype(F32)).astype(BF)
            G32[m][slot, mine] += RZ[m][slot, mine].astype(F32)

    def chip_send(ms, s):
        for m in ms:
            to_x(m, s).start()

    def out_copies(s):
        l, j = 1 - s // NC, s % NC
        for m in range(3):
            for at, cols in strips(m, l, j):
                src = OB[m].at[s % 2] if cols is None else OB[m].at[s % 2, :, cols]
                yield pltpu.make_async_copy(src, (og_o, ou_o, od_o)[m].at[at], o_s.at[m, s % 2])

    def out_wait(s):
        for m in range(3):
            pltpu.make_async_copy(OB[m].at[s % 2], OB[m].at[s % 2], o_s.at[m, s % 2]).wait()

    def last_wait(s):
        @pl.when(s >= 2)
        def _():
            out_wait(s)
        for m in range(3):
            to_x(m, s).wait_recv()

    def last_sum(slot, rx):
        for m in range(3):
            mine = pl.ds(m_of(c * QR[m], QR[m]), QR[m])
            OB[m][slot] = (G32[m][slot, mine] + RX[m][rx].astype(F32)).astype(BF)

    def last_out(s):
        for copy in out_copies(s):
            copy.start()

    def finish(s):
        last_wait(s)
        last_sum(s % 2, s % 4)
        last_out(s)

    def scale_of(wide):
        return lax.rsqrt(jnp.mean(wide * wide, -1, keepdims=True) + 1e-6)

    def norm(l):
        @pl.loop(0, T // 256)
        def _(t):
            rows = pl.ds(m_of(t * 256, 256), 256)
            wide = hb[0, rows, :].astype(F32)
            if l:
                h = (wide + acc[rows, :].astype(BF).astype(F32)).astype(BF)
                hb[1, rows, :] = h
                wide = h.astype(F32)
            a = (wide * scale_of(wide)).astype(BF)
            ab[rows, :] = a
            acc[rows, :] = jnp.zeros((256, D), F32)
            at = a.T
            for q in range(4):
                aT[l, pl.ds(pos(q) * Q, Q), rows] = at[q * Q:(q + 1) * Q]

    def gu_copies(j, t, out):
        rows = pl.ds(m_of(t * TB, TB), TB)
        for i, (v, h) in enumerate(((gst, g_h), (ust, u_h))):
            pair = (v.at[t], h.at[j, rows, :])
            yield pltpu.make_async_copy(*(pair if out else pair[::-1]), gu_s.at[i, t])

    def fwd_block(slot, j, t):
        rows = pl.ds(t * TB, TB)
        a = ab[rows, :]
        ps = []
        for n in range(0, FC, 256):
            g = dot(a, WG[slot, :, n:n + 256])
            u = dot(a, WU[slot, :, n:n + 256])
            gst[t, :, n:n + 256] = g
            ust[t, :, n:n + 256] = u
            ps.append((g * (1.0 / (1.0 + jnp.exp(-g))) * u).astype(BF))
        p = jnp.concatenate(ps, 1)
        for n in range(0, D, 256):
            acc[rows, n:n + 256] += dot(p, WD[slot, :, n:n + 256])

    def bwd_ab(slot, t, saved):
        rows = pl.ds(t * TB, TB)
        a = None if saved else ab[rows, :]
        dy = dyb[rows, :]
        for n in range(0, FC, 256):
            dp = dot_t(dy, WD[slot, n:n + 256, :]).astype(BF).astype(F32)
            if saved:
                g, u = gst[t, :, n:n + 256], ust[t, :, n:n + 256]
            else:
                g = dot(a, WG[slot, :, n:n + 256])
                u = dot(a, WU[slot, :, n:n + 256])
            sig = 1.0 / (1.0 + jnp.exp(-g))
            silu = g * sig
            p = (silu * u).astype(BF)
            pT[n:n + 256, rows] = p.T
            dub[rows, n:n + 256] = (dp * silu).astype(BF)
            dgb[rows, n:n + 256] = (dp * u * (sig * (1.0 + g * (1.0 - sig)))).astype(BF)

    def bwd_c(slot, t):
        for i in range(2):
            rows = pl.ds(t * TB + i * TB // 2, TB // 2)
            for n in range(0, D, 256):
                acc[rows, n:n + 256] += dot_t(dgb[rows, :], WG[slot, n:n + 256, :]) + dot_t(dub[rows, :], WU[slot, n:n + 256, :])

    def norm_back(l):
        @pl.loop(0, T // 256)
        def _(t):
            rows = pl.ds(m_of(t * 256, 256), 256)
            wide = hb[l, rows, :].astype(F32)
            sc = scale_of(wide)
            da = acc[rows, :].astype(BF).astype(F32)
            inner = jnp.sum(da * wide, -1, keepdims=True)
            dh = da * sc - wide * (sc * sc * sc * inner * (1.0 / D))
            acc[rows, :] = jnp.zeros((256, D), F32)
            dyb[rows, :] = (dyb[rows, :].astype(F32) + dh.astype(BF).astype(F32)).astype(BF)

    in_x = pltpu.make_async_copy(x_h, hb.at[0], io_s.at[0])
    in_dy = pltpu.make_async_copy(dy_h, dyb, io_s.at[1])
    in_x.start()
    in_dy.start()
    barrier = pltpu.get_barrier_semaphore()
    for dev in (xp, yp, zp):
        pl.semaphore_signal(barrier, inc=1, device_id=dev, device_id_type=MESH)
    pl.semaphore_wait(barrier, 3)
    send_x(0)
    send_ps(0)

    @pl.loop(1, NC)
    def _(s):
        send_x(s)
    in_x.wait()
    norm(0)
    in_dy.wait()
    stage1(0)
    stage1(1)
    stage2(0)
    ready(0)
    load(0)

    @pl.loop(0, NC)
    def _(j):
        loaded(j)
        send_x(NC + j)

        @pl.when(j == 0)
        def _():
            send_ps(1)

        for t in range(NB):
            @pl.when(j > 0)
            def _():
                for copy in gu_copies(j - 1, t, True):
                    copy.wait()
            fwd_block(j % 2, j, t)
            for copy in gu_copies(j, t, True):
                copy.start()
            if t == 0:
                stage1(j + 2)
            if t == 1:
                stage2(j + 1)
            if t == 2:
                ready(j + 1)
                load(j + 1)

    for t in range(NB):
        for copy in gu_copies(NC - 1, t, True):
            copy.wait()

    stage2(NC + 1)
    norm(1)

    for phase in range(2):
        if phase == 1:
            for t in range(NB):
                for copy in gu_copies(0, t, False):
                    copy.start()

        def when(yes):
            return lambda f: pl.when(yes)(f) if phase == 0 else f()

        @pl.loop(0, NC)
        def _(j):
            s = phase * NC + j
            step = NC + s
            slot = step % 2
            loaded(step)
            if phase == 1:
                for t in range(NB):
                    for copy in gu_copies(j, t, False):
                        copy.wait()
            bwd_ab(slot, 0, phase == 1)

            @when(s >= 1)
            def _():
                chip_wait(range(3), s - 1)
                chip_sum(range(3), (s + 1) % 2)
                chip_send(range(3), s - 1)

            if phase == 0:
                @pl.when(step + 2 < 2 * NC)
                def _():
                    stage1(step + 2)

                @pl.when(step + 1 < 2 * NC)
                def _():
                    ready(step + 1)

            @pl.when(step + 1 < 3 * NC)
            def _():
                load(step + 1)

            bwd_c(slot, 0)
            for t in range(1, NB):
                bwd_ab(slot, t, phase == 1)
                bwd_c(slot, t)

            @when(s >= 2)
            def _():
                last_wait(s - 2)

            if phase == 1:
                @pl.when(j + 1 < NC)
                def _():
                    for t in range(NB):
                        for copy in gu_copies(j + 1, t, False):
                            copy.start()

            last_sum(s % 2, (s + 2) % 4)
            grads_first(s % 2, 1 - phase)
            for m in (2, 0, 1):
                to_z(m, s).start()

            @when(s >= 2)
            def _():
                last_out(s - 2)

            grads_mine(s % 2, 1 - phase)

            if phase == 0:
                @pl.when(step + 2 < 2 * NC)
                def _():
                    stage2(step + 2)
        if phase == 0:
            norm_back(1)

    last = 2 * NC - 1
    chip_wait(range(3), last)
    chip_sum(range(3), last % 2)
    chip_send(range(3), last)
    norm_back(0)
    out_dx = pltpu.make_async_copy(dyb, dx_o, io_s.at[0])
    out_dx.start()
    drain_ag()
    finish(last - 1)
    finish(last)
    for s in (last - 1, last):
        for m in range(3):
            to_x(m, s).wait_send()
        out_wait(s)
    out_dx.wait()


def copy_kernel(*refs):
    n = (len(refs) - 2) // 3
    src, dst, held, s_in, s_out = refs[:n], refs[n:2 * n], refs[2 * n:3 * n], refs[-2], refs[-1]
    pieces = [(i, pl.ds(p * (src[i].shape[0] // 4), src[i].shape[0] // 4)) for i in range(n) for p in range(4)]
    ins = [pltpu.make_async_copy(src[i].at[r], held[i].at[r], s_in.at[x]) for x, (i, r) in enumerate(pieces)]
    outs = [pltpu.make_async_copy(held[i].at[r], dst[i].at[r], s_out.at[x]) for x, (i, r) in enumerate(pieces)]
    for copy in ins:
        copy.start()
    for x in range(len(pieces)):
        ins[x].wait()
        outs[x].start()
    for copy in outs:
        copy.wait()


def solution(mesh):
    def local(x, dy, wg, wu, wd):
        _, T, D = x.shape
        L, Q, F = wg.shape
        FD = wd.shape[1]
        NC = 6
        FC = F // NC
        S = FC // 4
        sds = jax.ShapeDtypeStruct
        hbm = pl.BlockSpec(memory_space=pltpu.HBM)
        V, DMA = pltpu.VMEM, pltpu.SemaphoreType.DMA
        gate, down = (L, NC, Q, FC), (L, NC, S, D)
        outs = [sds((T, D), BF), sds(wg.shape, BF), sds(wu.shape, BF), sds(wd.shape, BF)]
        outs += [sds(s, BF) for s in (gate, gate, down) * 2]
        outs += [sds(t.shape, BF) for t in (wg, wu, wd)]
        outs += [sds((NC, T, FC), F32)] * 2
        scratch = [V((2, T, D), BF), V((T, D), BF), V((T, D), BF), V((2, D, T), BF), V((T, D), F32),
                   V((2, D, FC), BF), V((2, D, FC), BF), V((2, FC, D), BF),
                   V((FC, T), BF), V((T, FC), BF), V((T, FC), BF),
                   V((T // TB, TB, FC), F32), V((T // TB, TB, FC), F32), DMA((2, T // TB))]
        h3 = ((2 * Q, FC), (2 * Q, FC), (2 * S, D))
        q3 = ((Q, FC), (Q, FC), (S, D))
        scratch += [V(s, BF) for s in h3] + [V((2, *s), BF) for s in h3] + [V((2, *s), F32) for s in h3]
        scratch += [V((2, *s), BF) for s in q3] + [V((4, *s), BF) for s in q3] + [V((2, *s), BF) for s in q3]
        LC = L * NC
        scratch += [DMA((2,)), DMA((3, 2)), DMA((3, L)), DMA((3, L)), DMA((3, LC)), DMA((3, LC)), DMA((3, LC)), DMA((3, LC)),
                    DMA((2, 3, LC)), DMA((2, 3, LC)), DMA((3,)), DMA((3, 2)), DMA((3, 2)), DMA((3, 4)), DMA((3, 2))]
        res = pl.pallas_call(
            functools.partial(kernel, NC),
            out_shape=outs,
            in_specs=[hbm] * 5,
            out_specs=[hbm] * len(outs),
            scratch_shapes=scratch,
            compiler_params=pltpu.CompilerParams(collective_id=0, has_side_effects=True, vmem_limit_bytes=67043328),
        )(x[0], dy[0], wg, wu, wd)
        grads = [t.reshape(-1, t.shape[-1]) for t in res[:4]]
        n = len(grads)
        dx, *dw = pl.pallas_call(
            copy_kernel,
            out_shape=[sds(t.shape, BF) for t in grads],
            in_specs=[hbm] * n,
            out_specs=[hbm] * n,
            scratch_shapes=[V(t.shape, BF) for t in grads] + [DMA((4 * n,)), DMA((4 * n,))],
        )(*grads)
        return (dx[None], *(t.reshape(w.shape) for t, w in zip(dw, (wg, wu, wd))))

    seq, w = P(("rep", "dp"), None, None), P(None, "dp", None)
    grad = P("rep", "dp", None)
    return jax.shard_map(local, mesh=mesh, in_specs=(seq, seq, w, w, w), out_specs=(seq, grad, grad, grad), check_vma=False)
```

```python
import functools

import jax
import jax.numpy as jnp
from jax import lax
from jax.experimental import pallas as pl
from jax.experimental.pallas import tpu as pltpu
from jax.sharding import PartitionSpec as P

BF, F32 = jnp.bfloat16, jnp.float32
MESH = pl.DeviceIdType.MESH
TB = 512


def pos(q):
    return (q % 2) * 2 + q // 2


def dot(a, b):
    return jnp.dot(a, b, preferred_element_type=F32)


def dot_t(a, b):
    return lax.dot_general(a, b, (((1,), (1,)), ((), ())), preferred_element_type=F32)


def kernel(NC, x_h, dy_h, wg_h, wu_h, wd_h,
           dx_o, og_o, ou_o, od_o, gxg, gxu, gxd, gdg, gdu, gdd, psg, psu, psd, g_h, u_h,
           hb, dyb, ab, aT, acc, WG, WU, WD, pT, dgb, dub, gst, ust, gu_s,
           szg, szu, szd, rzg, rzu, rzd, Gg, Gu, Gd, sxg, sxu, sxd, rxg, rxu, rxd, obg, obu, obd,
           io_s, ld_s, ps_s, ps_r, ax_s, ax_r, ay_s, ay_r, az_s, az_r,
           z_s, z_r, x_s, x_r, o_s):
    T, D = ab.shape
    FC = dgb.shape[1]
    L = wg_h.shape[0]
    Q = wg_h.shape[1]
    S = FC // 4
    FD = wd_h.shape[1]
    Q2, S2 = Q // 2, S // 2
    NB = T // TB
    r = lax.axis_index("rep")
    me = lax.axis_index("dp")
    c, k = me // 2, me % 2
    xp = {"rep": r, "dp": (1 - c) * 2 + k}
    yp = {"rep": 1 - r, "dp": me}
    zp = {"rep": r, "dp": c * 2 + 1 - k}
    zq = c * 2 + 1 - k
    xq = (1 - c) * 2 + k
    dq = (1 - c) * 2 + 1 - k

    def m_of(i, n):
        return pl.multiple_of(i, n)

    def remote(src, dst, ss, rs, dev):
        return pltpu.make_async_remote_copy(src, dst, ss, rs, device_id=dev, device_id_type=MESH)

    def half(m, h):
        n = S2 if m == 2 else Q2
        return pl.ds(m_of(h * n, n), n)

    W_in = (wg_h, wu_h, wd_h)
    GX, GD, PS, WV = (gxg, gxu, gxd), (gdg, gdu, gdd), (psg, psu, psd), (WG, WU, WD)

    def strips(m, l, j, h=None):
        if m == 2:
            n = S if h is None else S2
            at = j * S if h is None else j * S + h * S2
            return [((l, pl.ds(m_of(at, n), n), slice(None)), None)]
        rows = slice(None) if h is None else half(m, h)
        return [((l, rows, pl.ds(m_of(d * FD + j * S, S), S)), pl.ds(pos(d) * S, S)) for d in range(4)]

    def send_x(s):
        l, j = s // NC, s % NC
        for m in range(3):
            for src, cols in strips(m, l, j, r):
                dst = GX[m].at[l, j, half(m, r)] if cols is None else GX[m].at[l, j, half(m, r), cols]
                remote(W_in[m].at[src], dst, ax_s.at[m, s], ax_r.at[m, s], xp).start()

    def send_ps(l):
        for m in range(3):
            remote(W_in[m].at[l], PS[m].at[l], ps_s.at[m, l], ps_r.at[m, l], zp).start()

    def whole(m, s, h, ss, rs, dev, G=None):
        l, j = s // NC, s % NC
        src = GX[m].at[l, j, half(m, h)]
        return remote(src, (G or GX)[m].at[l, j, half(m, h)], ss, rs, dev)

    def stage1(s):
        for m in range(3):
            whole(m, s, r, ax_s.at[m, s], ax_r.at[m, s], xp).wait_recv()
            whole(m, s, r, ay_s.at[m, s], ay_r.at[m, s], yp).start()
            whole(m, s, r, az_s.at[0, m, s], az_r.at[0, m, s], zp, GD).start()

    def stage2(s):
        for m in range(3):
            whole(m, s, 1 - r, ay_s.at[m, s], ay_r.at[m, s], yp).wait_recv()
            whole(m, s, 1 - r, az_s.at[1, m, s], az_r.at[1, m, s], zp, GD).start()

    def ready(s):
        for i in range(2):
            for m in range(3):
                whole(m, s, r if i == 0 else 1 - r, az_s.at[i, m, s], az_r.at[i, m, s], zp, GD).wait_recv()

        @pl.when(s % NC == 0)
        def _():
            l = s // NC
            for m in range(3):
                remote(W_in[m].at[l], PS[m].at[l], ps_s.at[m, l], ps_r.at[m, l], zp).wait_recv()

    def drain_ag():
        @pl.loop(0, L * NC)
        def _(s):
            for m in range(3):
                whole(m, s, r, ax_s.at[m, s], ax_r.at[m, s], xp).wait_send()
                whole(m, s, r, ay_s.at[m, s], ay_r.at[m, s], yp).wait_send()
                for i in range(2):
                    whole(m, s, r, az_s.at[i, m, s], az_r.at[i, m, s], zp, GD).wait_send()
        for l in range(L):
            for m in range(3):
                remote(W_in[m].at[l], PS[m].at[l], ps_s.at[m, l], ps_r.at[m, l], zp).wait_send()

    def load(step):
        l, j, slot = (step // NC) % 2, step % NC, step % 2
        for m in range(3):
            for q, src in ((me, W_in[m]), (zq, PS[m])):
                for at, cols in strips(m, l, j):
                    if m == 2:
                        dst = WV[m].at[slot, pl.ds(m_of(((q % 2) * 2 + q // 2) * S, S), S)]
                    else:
                        dst = WV[m].at[slot, pl.ds(m_of(q * Q, Q), Q), cols]
                    pltpu.make_async_copy(src.at[at], dst, ld_s.at[m, slot]).start()
            for q, src in ((xq, GX[m]), (dq, GD[m])):
                if m == 2:
                    dst = WV[m].at[slot, pl.ds(m_of(((q % 2) * 2 + q // 2) * S, S), S)]
                else:
                    dst = WV[m].at[slot, pl.ds(m_of(q * Q, Q), Q)]
                pltpu.make_async_copy(src.at[l, j], dst, ld_s.at[m, slot]).start()

    def loaded(step):
        slot = step % 2
        for m in range(3):
            pltpu.make_async_copy(WV[m].at[slot], WV[m].at[slot], ld_s.at[m, slot]).wait()

    SZ, RZ, G32, SX, RX, OB = (szg, szu, szd), (rzg, rzu, rzd), (Gg, Gu, Gd), (sxg, sxu, sxd), (rxg, rxu, rxd), (obg, obu, obd)
    HR = (2 * Q, 2 * Q, 2 * S)
    QR = (Q, Q, S)

    def to_z(m, s):
        return remote(SZ[m], RZ[m].at[s % 2], z_s.at[m], z_r.at[m, s % 2], zp)

    def to_x(m, s):
        return remote(SX[m].at[s % 2], RX[m].at[s % 4], x_s.at[m, s % 2], x_r.at[m, s % 4], xp)

    def grads(m, part, n, l=0):
        rows = pl.ds(m_of(part * HR[m], HR[m]), HR[m])
        if m == 2:
            return dot(pT[rows, :], dyb[:, n:n + 256])
        return dot(aT[l, rows, :], (dgb, dub)[m][:, n:n + 256])

    def grads_first(slot, l):
        for n in range(0, D, 256):
            szd[:, n:n + 256] = grads(2, 1 - k, n).astype(BF)
            Gd[slot, :, n:n + 256] = grads(2, k, n)
        for m in (0, 1):
            for n in range(0, FC, 256):
                SZ[m][:, n:n + 256] = grads(m, 1 - k, n, l).astype(BF)

    def grads_mine(slot, l):
        for m in (0, 1):
            for n in range(0, FC, 256):
                G32[m][slot, :, n:n + 256] = grads(m, k, n, l)

    def chip_wait(ms, s):
        for m in ms:
            @pl.when(s >= 2)
            def _():
                to_x(m, s).wait_send()
            to_z(m, s).wait()

    def chip_sum(ms, slot):
        for m in ms:
            mine, other = pl.ds(m_of(c * QR[m], QR[m]), QR[m]), pl.ds(m_of((1 - c) * QR[m], QR[m]), QR[m])
            SX[m][slot] = (G32[m][slot, other] + RZ[m][slot, other].astype(F32)).astype(BF)
            G32[m][slot, mine] += RZ[m][slot, mine].astype(F32)

    def chip_send(ms, s):
        for m in ms:
            to_x(m, s).start()

    def out_copies(s):
        l, j = 1 - s // NC, s % NC
        for m in range(3):
            for at, cols in strips(m, l, j):
                src = OB[m].at[s % 2] if cols is None else OB[m].at[s % 2, :, cols]
                yield pltpu.make_async_copy(src, (og_o, ou_o, od_o)[m].at[at], o_s.at[m, s % 2])

    def out_wait(s):
        for m in range(3):
            pltpu.make_async_copy(OB[m].at[s % 2], OB[m].at[s % 2], o_s.at[m, s % 2]).wait()

    def last_wait(s):
        @pl.when(s >= 2)
        def _():
            out_wait(s)
        for m in range(3):
            to_x(m, s).wait_recv()

    def last_sum(slot, rx):
        for m in range(3):
            mine = pl.ds(m_of(c * QR[m], QR[m]), QR[m])
            OB[m][slot] = (G32[m][slot, mine] + RX[m][rx].astype(F32)).astype(BF)

    def last_out(s):
        for copy in out_copies(s):
            copy.start()

    def finish(s):
        last_wait(s)
        last_sum(s % 2, s % 4)
        last_out(s)

    def scale_of(wide):
        return lax.rsqrt(jnp.mean(wide * wide, -1, keepdims=True) + 1e-6)

    def norm(l):
        @pl.loop(0, T // 256)
        def _(t):
            rows = pl.ds(m_of(t * 256, 256), 256)
            wide = hb[0, rows, :].astype(F32)
            if l:
                h = (wide + acc[rows, :].astype(BF).astype(F32)).astype(BF)
                hb[1, rows, :] = h
                wide = h.astype(F32)
            a = (wide * scale_of(wide)).astype(BF)
            ab[rows, :] = a
            acc[rows, :] = jnp.zeros((256, D), F32)
            at = a.T
            for q in range(4):
                aT[l, pl.ds(pos(q) * Q, Q), rows] = at[q * Q:(q + 1) * Q]

    def gu_copies(j, t, out):
        rows = pl.ds(m_of(t * TB, TB), TB)
        for i, (v, h) in enumerate(((gst, g_h), (ust, u_h))):
            pair = (v.at[t], h.at[j, rows, :])
            yield pltpu.make_async_copy(*(pair if out else pair[::-1]), gu_s.at[i, t])

    def fwd_block(slot, j, t):
        rows = pl.ds(t * TB, TB)
        a = ab[rows, :]
        ps = []
        for n in range(0, FC, 256):
            g = dot(a, WG[slot, :, n:n + 256])
            u = dot(a, WU[slot, :, n:n + 256])
            gst[t, :, n:n + 256] = g
            ust[t, :, n:n + 256] = u
            ps.append((g * (1.0 / (1.0 + jnp.exp(-g))) * u).astype(BF))
        p = jnp.concatenate(ps, 1)
        for n in range(0, D, 256):
            acc[rows, n:n + 256] += dot(p, WD[slot, :, n:n + 256])

    def bwd_ab(slot, t, saved):
        rows = pl.ds(t * TB, TB)
        a = None if saved else ab[rows, :]
        dy = dyb[rows, :]
        for n in range(0, FC, 256):
            dp = dot_t(dy, WD[slot, n:n + 256, :]).astype(BF).astype(F32)
            if saved:
                g, u = gst[t, :, n:n + 256], ust[t, :, n:n + 256]
            else:
                g = dot(a, WG[slot, :, n:n + 256])
                u = dot(a, WU[slot, :, n:n + 256])
            sig = 1.0 / (1.0 + jnp.exp(-g))
            silu = g * sig
            p = (silu * u).astype(BF)
            pT[n:n + 256, rows] = p.T
            dub[rows, n:n + 256] = (dp * silu).astype(BF)
            dgb[rows, n:n + 256] = (dp * u * (sig * (1.0 + g * (1.0 - sig)))).astype(BF)

    def bwd_c(slot, t):
        for i in range(2):
            rows = pl.ds(t * TB + i * TB // 2, TB // 2)
            for n in range(0, D, 256):
                acc[rows, n:n + 256] += dot_t(dgb[rows, :], WG[slot, n:n + 256, :]) + dot_t(dub[rows, :], WU[slot, n:n + 256, :])

    def norm_back(l):
        @pl.loop(0, T // 256)
        def _(t):
            rows = pl.ds(m_of(t * 256, 256), 256)
            wide = hb[l, rows, :].astype(F32)
            sc = scale_of(wide)
            da = acc[rows, :].astype(BF).astype(F32)
            inner = jnp.sum(da * wide, -1, keepdims=True)
            dh = da * sc - wide * (sc * sc * sc * inner * (1.0 / D))
            acc[rows, :] = jnp.zeros((256, D), F32)
            dyb[rows, :] = (dyb[rows, :].astype(F32) + dh.astype(BF).astype(F32)).astype(BF)

    in_x = pltpu.make_async_copy(x_h, hb.at[0], io_s.at[0])
    in_dy = pltpu.make_async_copy(dy_h, dyb, io_s.at[1])
    in_x.start()
    in_dy.start()
    barrier = pltpu.get_barrier_semaphore()
    for dev in (xp, yp, zp):
        pl.semaphore_signal(barrier, inc=1, device_id=dev, device_id_type=MESH)
    pl.semaphore_wait(barrier, 3)
    send_x(0)
    send_ps(0)

    @pl.loop(1, NC)
    def _(s):
        send_x(s)
    in_x.wait()
    norm(0)
    in_dy.wait()
    stage1(0)
    stage1(1)
    stage2(0)
    ready(0)
    load(0)

    @pl.loop(0, NC)
    def _(j):
        loaded(j)
        send_x(NC + j)

        @pl.when(j == 0)
        def _():
            send_ps(1)

        for t in range(NB):
            @pl.when(j > 0)
            def _():
                for copy in gu_copies(j - 1, t, True):
                    copy.wait()
            fwd_block(j % 2, j, t)
            for copy in gu_copies(j, t, True):
                copy.start()
            if t == 0:
                stage1(j + 2)
            if t == 1:
                stage2(j + 1)
            if t == 2:
                ready(j + 1)
                load(j + 1)

    for t in range(NB):
        for copy in gu_copies(NC - 1, t, True):
            copy.wait()

    stage2(NC + 1)
    norm(1)

    for phase in range(2):
        if phase == 1:
            for t in range(NB):
                for copy in gu_copies(0, t, False):
                    copy.start()

        def when(yes):
            return lambda f: pl.when(yes)(f) if phase == 0 else f()

        @pl.loop(0, NC)
        def _(j):
            s = phase * NC + j
            step = NC + s
            slot = step % 2
            loaded(step)
            if phase == 1:
                for t in range(NB):
                    for copy in gu_copies(j, t, False):
                        copy.wait()
            bwd_ab(slot, 0, phase == 1)
            bwd_c(slot, 0)
            bwd_ab(slot, 1, phase == 1)

            @when(s >= 1)
            def _():
                chip_wait(range(3), s - 1)
                chip_sum(range(3), (s + 1) % 2)
                chip_send(range(3), s - 1)

            if phase == 0:
                @pl.when(step + 2 < 2 * NC)
                def _():
                    stage1(step + 2)

                @pl.when(step + 1 < 2 * NC)
                def _():
                    ready(step + 1)

            @pl.when(step + 1 < 3 * NC)
            def _():
                load(step + 1)

            bwd_c(slot, 1)
            for t in range(2, NB):
                bwd_ab(slot, t, phase == 1)
                bwd_c(slot, t)

            @when(s >= 2)
            def _():
                last_wait(s - 2)

            if phase == 1:
                @pl.when(j + 1 < NC)
                def _():
                    for t in range(NB):
                        for copy in gu_copies(j + 1, t, False):
                            copy.start()

            last_sum(s % 2, (s + 2) % 4)
            grads_first(s % 2, 1 - phase)
            for m in (2, 0, 1):
                to_z(m, s).start()

            @when(s >= 2)
            def _():
                last_out(s - 2)

            grads_mine(s % 2, 1 - phase)

            if phase == 0:
                @pl.when(step + 2 < 2 * NC)
                def _():
                    stage2(step + 2)
        if phase == 0:
            norm_back(1)

    last = 2 * NC - 1
    chip_wait(range(3), last)
    chip_sum(range(3), last % 2)
    chip_send(range(3), last)
    norm_back(0)
    out_dx = pltpu.make_async_copy(dyb, dx_o, io_s.at[0])
    out_dx.start()
    drain_ag()
    finish(last - 1)
    finish(last)
    for s in (last - 1, last):
        for m in range(3):
            to_x(m, s).wait_send()
        out_wait(s)
    out_dx.wait()


def copy_kernel(*refs):
    n = (len(refs) - 2) // 3
    src, dst, held, s_in, s_out = refs[:n], refs[n:2 * n], refs[2 * n:3 * n], refs[-2], refs[-1]
    pieces = [(i, pl.ds(p * (src[i].shape[0] // 4), src[i].shape[0] // 4)) for i in range(n) for p in range(4)]
    ins = [pltpu.make_async_copy(src[i].at[r], held[i].at[r], s_in.at[x]) for x, (i, r) in enumerate(pieces)]
    outs = [pltpu.make_async_copy(held[i].at[r], dst[i].at[r], s_out.at[x]) for x, (i, r) in enumerate(pieces)]
    for copy in ins:
        copy.start()
    for x in range(len(pieces)):
        ins[x].wait()
        outs[x].start()
    for copy in outs:
        copy.wait()


def solution(mesh):
    def local(x, dy, wg, wu, wd):
        _, T, D = x.shape
        L, Q, F = wg.shape
        FD = wd.shape[1]
        NC = 6
        FC = F // NC
        S = FC // 4
        sds = jax.ShapeDtypeStruct
        hbm = pl.BlockSpec(memory_space=pltpu.HBM)
        V, DMA = pltpu.VMEM, pltpu.SemaphoreType.DMA
        gate, down = (L, NC, Q, FC), (L, NC, S, D)
        outs = [sds((T, D), BF), sds(wg.shape, BF), sds(wu.shape, BF), sds(wd.shape, BF)]
        outs += [sds(s, BF) for s in (gate, gate, down) * 2]
        outs += [sds(t.shape, BF) for t in (wg, wu, wd)]
        outs += [sds((NC, T, FC), F32)] * 2
        scratch = [V((2, T, D), BF), V((T, D), BF), V((T, D), BF), V((2, D, T), BF), V((T, D), F32),
                   V((2, D, FC), BF), V((2, D, FC), BF), V((2, FC, D), BF),
                   V((FC, T), BF), V((T, FC), BF), V((T, FC), BF),
                   V((T // TB, TB, FC), F32), V((T // TB, TB, FC), F32), DMA((2, T // TB))]
        h3 = ((2 * Q, FC), (2 * Q, FC), (2 * S, D))
        q3 = ((Q, FC), (Q, FC), (S, D))
        scratch += [V(s, BF) for s in h3] + [V((2, *s), BF) for s in h3] + [V((2, *s), F32) for s in h3]
        scratch += [V((2, *s), BF) for s in q3] + [V((4, *s), BF) for s in q3] + [V((2, *s), BF) for s in q3]
        LC = L * NC
        scratch += [DMA((2,)), DMA((3, 2)), DMA((3, L)), DMA((3, L)), DMA((3, LC)), DMA((3, LC)), DMA((3, LC)), DMA((3, LC)),
                    DMA((2, 3, LC)), DMA((2, 3, LC)), DMA((3,)), DMA((3, 2)), DMA((3, 2)), DMA((3, 4)), DMA((3, 2))]
        res = pl.pallas_call(
            functools.partial(kernel, NC),
            out_shape=outs,
            in_specs=[hbm] * 5,
            out_specs=[hbm] * len(outs),
            scratch_shapes=scratch,
            compiler_params=pltpu.CompilerParams(collective_id=0, has_side_effects=True, vmem_limit_bytes=67043328),
        )(x[0], dy[0], wg, wu, wd)
        grads = [t.reshape(-1, t.shape[-1]) for t in res[:4]]
        n = len(grads)
        dx, *dw = pl.pallas_call(
            copy_kernel,
            out_shape=[sds(t.shape, BF) for t in grads],
            in_specs=[hbm] * n,
            out_specs=[hbm] * n,
            scratch_shapes=[V(t.shape, BF) for t in grads] + [DMA((4 * n,)), DMA((4 * n,))],
        )(*grads)
        return (dx[None], *(t.reshape(w.shape) for t, w in zip(dw, (wg, wu, wd))))

    seq, w = P(("rep", "dp"), None, None), P(None, "dp", None)
    grad = P("rep", "dp", None)
    return jax.shard_map(local, mesh=mesh, in_specs=(seq, seq, w, w, w), out_specs=(seq, grad, grad, grad), check_vma=False)
```

```python
import functools

import jax
import jax.numpy as jnp
from jax import lax
from jax.experimental import pallas as pl
from jax.experimental.pallas import tpu as pltpu
from jax.sharding import PartitionSpec as P

BF, F32 = jnp.bfloat16, jnp.float32
MESH = pl.DeviceIdType.MESH
TB = 512


def pos(q):
    return (q % 2) * 2 + q // 2


def dot(a, b):
    return jnp.dot(a, b, preferred_element_type=F32)


def dot_t(a, b):
    return lax.dot_general(a, b, (((1,), (1,)), ((), ())), preferred_element_type=F32)


def kernel(NC, x_h, dy_h, wg_h, wu_h, wd_h,
           dx_o, og_o, ou_o, od_o, gxg, gxu, gxd, gdg, gdu, gdd, psg, psu, psd, g_h, u_h,
           hb, dyb, ab, aT, acc, WG, WU, WD, pT, dgb, dub, gst, ust, gu_s,
           szg, szu, szd, rzg, rzu, rzd, Gg, Gu, Gd, sxg, sxu, sxd, rxg, rxu, rxd, obg, obu, obd,
           io_s, ld_s, ps_s, ps_r, ax_s, ax_r, ay_s, ay_r, az_s, az_r,
           z_s, z_r, x_s, x_r, o_s):
    T, D = ab.shape
    FC = dgb.shape[1]
    L = wg_h.shape[0]
    Q = wg_h.shape[1]
    S = FC // 4
    FD = wd_h.shape[1]
    Q2, S2 = Q // 2, S // 2
    NB = T // TB
    r = lax.axis_index("rep")
    me = lax.axis_index("dp")
    c, k = me // 2, me % 2
    xp = {"rep": r, "dp": (1 - c) * 2 + k}
    yp = {"rep": 1 - r, "dp": me}
    zp = {"rep": r, "dp": c * 2 + 1 - k}
    zq = c * 2 + 1 - k
    xq = (1 - c) * 2 + k
    dq = (1 - c) * 2 + 1 - k

    def m_of(i, n):
        return pl.multiple_of(i, n)

    def remote(src, dst, ss, rs, dev):
        return pltpu.make_async_remote_copy(src, dst, ss, rs, device_id=dev, device_id_type=MESH)

    def half(m, h):
        n = S2 if m == 2 else Q2
        return pl.ds(m_of(h * n, n), n)

    W_in = (wg_h, wu_h, wd_h)
    GX, GD, PS, WV = (gxg, gxu, gxd), (gdg, gdu, gdd), (psg, psu, psd), (WG, WU, WD)

    def strips(m, l, j, h=None):
        if m == 2:
            n = S if h is None else S2
            at = j * S if h is None else j * S + h * S2
            return [((l, pl.ds(m_of(at, n), n), slice(None)), None)]
        rows = slice(None) if h is None else half(m, h)
        return [((l, rows, pl.ds(m_of(d * FD + j * S, S), S)), pl.ds(pos(d) * S, S)) for d in range(4)]

    def send_x(s):
        l, j = s // NC, s % NC
        for m in range(3):
            for src, cols in strips(m, l, j, r):
                dst = GX[m].at[l, j, half(m, r)] if cols is None else GX[m].at[l, j, half(m, r), cols]
                remote(W_in[m].at[src], dst, ax_s.at[m, s], ax_r.at[m, s], xp).start()

    def send_ps(l):
        for m in range(3):
            remote(W_in[m].at[l], PS[m].at[l], ps_s.at[m, l], ps_r.at[m, l], zp).start()

    def whole(m, s, h, ss, rs, dev, G=None):
        l, j = s // NC, s % NC
        src = GX[m].at[l, j, half(m, h)]
        return remote(src, (G or GX)[m].at[l, j, half(m, h)], ss, rs, dev)

    def stage1(s):
        for m in range(3):
            whole(m, s, r, ax_s.at[m, s], ax_r.at[m, s], xp).wait_recv()
            whole(m, s, r, ay_s.at[m, s], ay_r.at[m, s], yp).start()
            whole(m, s, r, az_s.at[0, m, s], az_r.at[0, m, s], zp, GD).start()

    def stage2(s):
        for m in range(3):
            whole(m, s, 1 - r, ay_s.at[m, s], ay_r.at[m, s], yp).wait_recv()
            whole(m, s, 1 - r, az_s.at[1, m, s], az_r.at[1, m, s], zp, GD).start()

    def ready(s):
        for i in range(2):
            for m in range(3):
                whole(m, s, r if i == 0 else 1 - r, az_s.at[i, m, s], az_r.at[i, m, s], zp, GD).wait_recv()

        @pl.when(s % NC == 0)
        def _():
            l = s // NC
            for m in range(3):
                remote(W_in[m].at[l], PS[m].at[l], ps_s.at[m, l], ps_r.at[m, l], zp).wait_recv()

    def drain_ag():
        @pl.loop(0, L * NC)
        def _(s):
            for m in range(3):
                whole(m, s, r, ax_s.at[m, s], ax_r.at[m, s], xp).wait_send()
                whole(m, s, r, ay_s.at[m, s], ay_r.at[m, s], yp).wait_send()
                for i in range(2):
                    whole(m, s, r, az_s.at[i, m, s], az_r.at[i, m, s], zp, GD).wait_send()
        for l in range(L):
            for m in range(3):
                remote(W_in[m].at[l], PS[m].at[l], ps_s.at[m, l], ps_r.at[m, l], zp).wait_send()

    def load(step):
        l, j, slot = (step // NC) % 2, step % NC, step % 2
        for m in range(3):
            for q, src in ((me, W_in[m]), (zq, PS[m])):
                for at, cols in strips(m, l, j):
                    if m == 2:
                        dst = WV[m].at[slot, pl.ds(m_of(((q % 2) * 2 + q // 2) * S, S), S)]
                    else:
                        dst = WV[m].at[slot, pl.ds(m_of(q * Q, Q), Q), cols]
                    pltpu.make_async_copy(src.at[at], dst, ld_s.at[m, slot]).start()
            for q, src in ((xq, GX[m]), (dq, GD[m])):
                if m == 2:
                    dst = WV[m].at[slot, pl.ds(m_of(((q % 2) * 2 + q // 2) * S, S), S)]
                else:
                    dst = WV[m].at[slot, pl.ds(m_of(q * Q, Q), Q)]
                pltpu.make_async_copy(src.at[l, j], dst, ld_s.at[m, slot]).start()

    def loaded(step):
        slot = step % 2
        for m in range(3):
            pltpu.make_async_copy(WV[m].at[slot], WV[m].at[slot], ld_s.at[m, slot]).wait()

    SZ, RZ, G32, SX, RX, OB = (szg, szu, szd), (rzg, rzu, rzd), (Gg, Gu, Gd), (sxg, sxu, sxd), (rxg, rxu, rxd), (obg, obu, obd)
    HR = (2 * Q, 2 * Q, 2 * S)
    QR = (Q, Q, S)

    def to_z(m, s):
        return remote(SZ[m], RZ[m].at[s % 2], z_s.at[m], z_r.at[m, s % 2], zp)

    def to_x(m, s):
        return remote(SX[m].at[s % 2], RX[m].at[s % 4], x_s.at[m, s % 2], x_r.at[m, s % 4], xp)

    def grads(m, part, n, l=0):
        rows = pl.ds(m_of(part * HR[m], HR[m]), HR[m])
        if m == 2:
            return dot(pT[rows, :], dyb[:, n:n + 256])
        return dot(aT[l, rows, :], (dgb, dub)[m][:, n:n + 256])

    def grads_first(slot, l):
        for n in range(0, D, 256):
            szd[:, n:n + 256] = grads(2, 1 - k, n).astype(BF)
            Gd[slot, :, n:n + 256] = grads(2, k, n)
        for m in (0, 1):
            for n in range(0, FC, 256):
                SZ[m][:, n:n + 256] = grads(m, 1 - k, n, l).astype(BF)

    def grads_mine(slot, l):
        for m in (0, 1):
            for n in range(0, FC, 256):
                G32[m][slot, :, n:n + 256] = grads(m, k, n, l)

    def chip_wait(ms, s):
        for m in ms:
            @pl.when(s >= 2)
            def _():
                to_x(m, s).wait_send()
            to_z(m, s).wait()

    def chip_sum(ms, slot):
        for m in ms:
            mine, other = pl.ds(m_of(c * QR[m], QR[m]), QR[m]), pl.ds(m_of((1 - c) * QR[m], QR[m]), QR[m])
            SX[m][slot] = (G32[m][slot, other] + RZ[m][slot, other].astype(F32)).astype(BF)
            G32[m][slot, mine] += RZ[m][slot, mine].astype(F32)

    def chip_send(ms, s):
        for m in ms:
            to_x(m, s).start()

    def out_copies(s):
        l, j = 1 - s // NC, s % NC
        for m in range(3):
            for at, cols in strips(m, l, j):
                src = OB[m].at[s % 2] if cols is None else OB[m].at[s % 2, :, cols]
                yield pltpu.make_async_copy(src, (og_o, ou_o, od_o)[m].at[at], o_s.at[m, s % 2])

    def out_wait(s):
        for m in range(3):
            pltpu.make_async_copy(OB[m].at[s % 2], OB[m].at[s % 2], o_s.at[m, s % 2]).wait()

    def last_wait(s):
        @pl.when(s >= 2)
        def _():
            out_wait(s)
        for m in range(3):
            to_x(m, s).wait_recv()

    def last_sum(slot, rx):
        for m in range(3):
            mine = pl.ds(m_of(c * QR[m], QR[m]), QR[m])
            OB[m][slot] = (G32[m][slot, mine] + RX[m][rx].astype(F32)).astype(BF)

    def last_out(s):
        for copy in out_copies(s):
            copy.start()

    def finish(s):
        last_wait(s)
        last_sum(s % 2, s % 4)
        last_out(s)

    def scale_of(wide):
        return lax.rsqrt(jnp.mean(wide * wide, -1, keepdims=True) + 1e-6)

    def norm(l):
        @pl.loop(0, T // 256)
        def _(t):
            rows = pl.ds(m_of(t * 256, 256), 256)
            wide = hb[0, rows, :].astype(F32)
            if l:
                h = (wide + acc[rows, :].astype(BF).astype(F32)).astype(BF)
                hb[1, rows, :] = h
                wide = h.astype(F32)
            a = (wide * scale_of(wide)).astype(BF)
            ab[rows, :] = a
            acc[rows, :] = jnp.zeros((256, D), F32)
            at = a.T
            for q in range(4):
                aT[l, pl.ds(pos(q) * Q, Q), rows] = at[q * Q:(q + 1) * Q]

    def gu_copies(j, t, out):
        rows = pl.ds(m_of(t * TB, TB), TB)
        for i, (v, h) in enumerate(((gst, g_h), (ust, u_h))):
            pair = (v.at[t], h.at[j, rows, :])
            yield pltpu.make_async_copy(*(pair if out else pair[::-1]), gu_s.at[i, t])

    def fwd_block(slot, j, t):
        rows = pl.ds(t * TB, TB)
        a = ab[rows, :]
        ps = []
        for n in range(0, FC, 256):
            g = dot(a, WG[slot, :, n:n + 256])
            u = dot(a, WU[slot, :, n:n + 256])
            gst[t, :, n:n + 256] = g
            ust[t, :, n:n + 256] = u
            ps.append((g * (1.0 / (1.0 + jnp.exp(-g))) * u).astype(BF))
        p = jnp.concatenate(ps, 1)
        for n in range(0, D, 256):
            acc[rows, n:n + 256] += dot(p, WD[slot, :, n:n + 256])

    def bwd_ab(slot, t, saved):
        rows = pl.ds(t * TB, TB)
        a = None if saved else ab[rows, :]
        dy = dyb[rows, :]
        for n in range(0, FC, 256):
            dp = dot_t(dy, WD[slot, n:n + 256, :]).astype(BF).astype(F32)
            if saved:
                g, u = gst[t, :, n:n + 256], ust[t, :, n:n + 256]
            else:
                g = dot(a, WG[slot, :, n:n + 256])
                u = dot(a, WU[slot, :, n:n + 256])
            sig = 1.0 / (1.0 + jnp.exp(-g))
            silu = g * sig
            p = (silu * u).astype(BF)
            pT[n:n + 256, rows] = p.T
            dub[rows, n:n + 256] = (dp * silu).astype(BF)
            dgb[rows, n:n + 256] = (dp * u * (sig * (1.0 + g * (1.0 - sig)))).astype(BF)

    def bwd_c(slot, t):
        for i in range(2):
            rows = pl.ds(t * TB + i * TB // 2, TB // 2)
            for n in range(0, D, 256):
                acc[rows, n:n + 256] += dot_t(dgb[rows, :], WG[slot, n:n + 256, :]) + dot_t(dub[rows, :], WU[slot, n:n + 256, :])

    def norm_back(l):
        @pl.loop(0, T // 256)
        def _(t):
            rows = pl.ds(m_of(t * 256, 256), 256)
            wide = hb[l, rows, :].astype(F32)
            sc = scale_of(wide)
            da = acc[rows, :].astype(BF).astype(F32)
            inner = jnp.sum(da * wide, -1, keepdims=True)
            dh = da * sc - wide * (sc * sc * sc * inner * (1.0 / D))
            acc[rows, :] = jnp.zeros((256, D), F32)
            dyb[rows, :] = (dyb[rows, :].astype(F32) + dh.astype(BF).astype(F32)).astype(BF)

    in_x = pltpu.make_async_copy(x_h, hb.at[0], io_s.at[0])
    in_dy = pltpu.make_async_copy(dy_h, dyb, io_s.at[1])
    in_x.start()
    in_dy.start()
    barrier = pltpu.get_barrier_semaphore()
    for dev in (xp, yp, zp):
        pl.semaphore_signal(barrier, inc=1, device_id=dev, device_id_type=MESH)
    pl.semaphore_wait(barrier, 3)
    send_x(0)
    send_ps(0)

    @pl.loop(1, NC)
    def _(s):
        send_x(s)
    in_x.wait()
    norm(0)
    in_dy.wait()
    stage1(0)
    stage1(1)
    stage2(0)
    ready(0)
    load(0)

    @pl.loop(0, NC)
    def _(j):
        loaded(j)
        send_x(NC + j)

        @pl.when(j == 0)
        def _():
            send_ps(1)

        for ts in ((0, 1), (2,), (3,)):
            t = ts[-1]

            @pl.when(j > 0)
            def _():
                for i in ts:
                    for copy in gu_copies(j - 1, i, True):
                        copy.wait()
            for i in ts:
                fwd_block(j % 2, j, i)
            for i in ts:
                for copy in gu_copies(j, i, True):
                    copy.start()
            if t == 1:
                stage1(j + 2)
                stage2(j + 1)
            if t == 2:
                ready(j + 1)
                load(j + 1)

    for t in range(NB):
        for copy in gu_copies(NC - 1, t, True):
            copy.wait()

    stage2(NC + 1)
    norm(1)

    for phase in range(2):
        if phase == 1:
            for t in range(NB):
                for copy in gu_copies(0, t, False):
                    copy.start()

        def when(yes):
            return lambda f: pl.when(yes)(f) if phase == 0 else f()

        @pl.loop(0, NC)
        def _(j):
            s = phase * NC + j
            step = NC + s
            slot = step % 2
            loaded(step)
            if phase == 1:
                for t in range(NB):
                    for copy in gu_copies(j, t, False):
                        copy.wait()
            bwd_ab(slot, 0, phase == 1)

            @when(s >= 1)
            def _():
                chip_wait(range(3), s - 1)
                chip_sum(range(3), (s + 1) % 2)
                chip_send(range(3), s - 1)

            if phase == 0:
                @pl.when(step + 2 < 2 * NC)
                def _():
                    stage1(step + 2)

                @pl.when(step + 1 < 2 * NC)
                def _():
                    ready(step + 1)

            @pl.when(step + 1 < 3 * NC)
            def _():
                load(step + 1)

            bwd_c(slot, 0)
            for t in range(1, NB):
                bwd_ab(slot, t, phase == 1)
                bwd_c(slot, t)

            @when(s >= 2)
            def _():
                last_wait(s - 2)

            if phase == 1:
                @pl.when(j + 1 < NC)
                def _():
                    for t in range(NB):
                        for copy in gu_copies(j + 1, t, False):
                            copy.start()

            last_sum(s % 2, (s + 2) % 4)
            grads_first(s % 2, 1 - phase)
            for m in (2, 0, 1):
                to_z(m, s).start()

            @when(s >= 2)
            def _():
                last_out(s - 2)

            grads_mine(s % 2, 1 - phase)

            if phase == 0:
                @pl.when(step + 2 < 2 * NC)
                def _():
                    stage2(step + 2)
        if phase == 0:
            norm_back(1)

    last = 2 * NC - 1
    chip_wait(range(3), last)
    chip_sum(range(3), last % 2)
    chip_send(range(3), last)
    norm_back(0)
    out_dx = pltpu.make_async_copy(dyb, dx_o, io_s.at[0])
    out_dx.start()
    drain_ag()
    finish(last - 1)
    finish(last)
    for s in (last - 1, last):
        for m in range(3):
            to_x(m, s).wait_send()
        out_wait(s)
    out_dx.wait()


def copy_kernel(*refs):
    n = (len(refs) - 2) // 3
    src, dst, held, s_in, s_out = refs[:n], refs[n:2 * n], refs[2 * n:3 * n], refs[-2], refs[-1]
    pieces = [(i, pl.ds(p * (src[i].shape[0] // 4), src[i].shape[0] // 4)) for i in range(n) for p in range(4)]
    ins = [pltpu.make_async_copy(src[i].at[r], held[i].at[r], s_in.at[x]) for x, (i, r) in enumerate(pieces)]
    outs = [pltpu.make_async_copy(held[i].at[r], dst[i].at[r], s_out.at[x]) for x, (i, r) in enumerate(pieces)]
    for copy in ins:
        copy.start()
    for x in range(len(pieces)):
        ins[x].wait()
        outs[x].start()
    for copy in outs:
        copy.wait()


def solution(mesh):
    def local(x, dy, wg, wu, wd):
        _, T, D = x.shape
        L, Q, F = wg.shape
        FD = wd.shape[1]
        NC = 6
        FC = F // NC
        S = FC // 4
        sds = jax.ShapeDtypeStruct
        hbm = pl.BlockSpec(memory_space=pltpu.HBM)
        V, DMA = pltpu.VMEM, pltpu.SemaphoreType.DMA
        gate, down = (L, NC, Q, FC), (L, NC, S, D)
        outs = [sds((T, D), BF), sds(wg.shape, BF), sds(wu.shape, BF), sds(wd.shape, BF)]
        outs += [sds(s, BF) for s in (gate, gate, down) * 2]
        outs += [sds(t.shape, BF) for t in (wg, wu, wd)]
        outs += [sds((NC, T, FC), F32)] * 2
        scratch = [V((2, T, D), BF), V((T, D), BF), V((T, D), BF), V((2, D, T), BF), V((T, D), F32),
                   V((2, D, FC), BF), V((2, D, FC), BF), V((2, FC, D), BF),
                   V((FC, T), BF), V((T, FC), BF), V((T, FC), BF),
                   V((T // TB, TB, FC), F32), V((T // TB, TB, FC), F32), DMA((2, T // TB))]
        h3 = ((2 * Q, FC), (2 * Q, FC), (2 * S, D))
        q3 = ((Q, FC), (Q, FC), (S, D))
        scratch += [V(s, BF) for s in h3] + [V((2, *s), BF) for s in h3] + [V((2, *s), F32) for s in h3]
        scratch += [V((2, *s), BF) for s in q3] + [V((4, *s), BF) for s in q3] + [V((2, *s), BF) for s in q3]
        LC = L * NC
        scratch += [DMA((2,)), DMA((3, 2)), DMA((3, L)), DMA((3, L)), DMA((3, LC)), DMA((3, LC)), DMA((3, LC)), DMA((3, LC)),
                    DMA((2, 3, LC)), DMA((2, 3, LC)), DMA((3,)), DMA((3, 2)), DMA((3, 2)), DMA((3, 4)), DMA((3, 2))]
        res = pl.pallas_call(
            functools.partial(kernel, NC),
            out_shape=outs,
            in_specs=[hbm] * 5,
            out_specs=[hbm] * len(outs),
            scratch_shapes=scratch,
            compiler_params=pltpu.CompilerParams(collective_id=0, has_side_effects=True, vmem_limit_bytes=67043328),
        )(x[0], dy[0], wg, wu, wd)
        grads = [t.reshape(-1, t.shape[-1]) for t in res[:4]]
        n = len(grads)
        dx, *dw = pl.pallas_call(
            copy_kernel,
            out_shape=[sds(t.shape, BF) for t in grads],
            in_specs=[hbm] * n,
            out_specs=[hbm] * n,
            scratch_shapes=[V(t.shape, BF) for t in grads] + [DMA((4 * n,)), DMA((4 * n,))],
        )(*grads)
        return (dx[None], *(t.reshape(w.shape) for t, w in zip(dw, (wg, wu, wd))))

    seq, w = P(("rep", "dp"), None, None), P(None, "dp", None)
    grad = P("rep", "dp", None)
    return jax.shard_map(local, mesh=mesh, in_specs=(seq, seq, w, w, w), out_specs=(seq, grad, grad, grad), check_vma=False)
```
